256 devices in a mesh: member: 4 (over x, y), lon: 32 (over z), lat: 2 (over core).
Axes of the slice: x: 2, y: 2, z: 32, core: 2. Of those that a mesh axis runs over, the one named last changes fastest.
The devices are a block of a 4x8x32 slice.
Arguments:
- strain_rate: float32 [3, 1024, 2160], P(None, 'lon', 'lat'), may hold values from -6 to 6
- stress_start: float32 [3, 1024, 2160], P(None, 'lon', 'lat'), may hold values from -3 to 3
- concentration: float32 [1024, 2160], P('lon', 'lat'), may hold values from 0.5 to 1
- cell_class: int32 [4096, 2160], P(('member', 'lon'), 'lat'), parts along dimension 0, may hold values from 0 to 7
- land_mask: int32 [1024, 2160], P('lon', 'lat'), may hold values 0 or 1
- fold_partner: int32 [1024], replicated, may hold values from 0 to 1023, each once
- kernel_weights: float32 [7, 7], replicated, may hold values from 0.05 to 0.5
Outputs:
- stress_out: float32 [3, 4096, 2160], P(None, ('member', 'lon'), 'lat'), parts along dimension 1
- damage_out: float32 [4096, 2160], P(('member', 'lon'), 'lat'), parts along dimension 0
- mean_overstress: float32 [12], P('member'), parts along dimension 0
The draws below stay inside these ranges and needn't reach their ends.
There are 4 independent parts, one for each index of `member`. The reference program is written for one: setup_inputs(seed, part) draws one part's arguments, and reference() takes and returns one part's arrays. A program takes and returns all parts, laid end to end along the dimension named above; an argument that names none is the same for every part. Nothing has to cross between parts.
Inputs may be any that keep to these rules, and one draw needn't show every extreme that they name: `fold_partner`: each of the 1024 longitude indices appears once.
All inputs are finite; a program needn't handle non-finite values. No bound on the sum of `land_mask` on one device may be relied on, other than what follows from the above.
Results may differ from the reference program's by a relative error of at most 0.0001.
Values sent between devices are 32-bit elements; how exact they have to be, the bound alone decides.
No kernel may reach another device: no remote copies, remote signals or barrier semaphores. Data moves between devices by JAX's collectives and lax.ppermute only.
A program may use at most 64 MiB of HBM per device.

```python
import math
import jax
import jax.numpy as jnp

ITERS = 3
KW = 7
NLON = 1024
NLAT = 2160


def set_ends(result, key, least, top_value):
    longest = result.shape.index(max(result.shape))
    spots = []
    for shift in (0, 1):
        where = [jax.random.randint(jax.random.fold_in(key, axis), (), 0, length) for axis, length in enumerate(result.shape)]
        where[longest] = (where[longest] + shift) % result.shape[longest]
        spots.append(tuple(where))
    return result.at[spots[0]].set(least).at[spots[1]].set(top_value)


def shard_levels(own_key, extent, shards, low, top_value):
    def one(position, blocks):
        steps = jax.random.uniform(jax.random.fold_in(jax.random.fold_in(own_key, 6), position), (blocks,), jnp.float32, low / len(shards), top_value / len(shards))
        return jnp.repeat(jnp.exp(steps), extent[position] // blocks).reshape((-1,) + (1,) * (len(extent) - position - 1))

    gain = one(*shards[0])
    for cut in shards[1:]:
        gain = gain * one(*cut)
    return gain


def scatter_about(stream_key, extent, scale, most, pieces=(), dtype=jnp.bfloat16):
    gain = shard_levels(stream_key, extent, pieces, -0.22, 0.18) if pieces else 1.0
    values = jax.random.normal(stream_key, extent, jnp.float32) * scale * gain
    return jnp.minimum(jnp.maximum(values, -most), most).astype(dtype)


def setup_inputs(seed: int = 0, part: int = 0) -> dict:
    streams_of = jax.random.split(jax.random.key(seed), 8)
    part_splits = jax.random.split(jax.random.fold_in(streams_of[7], part), 8)
    return {
        "strain_rate": scatter_about(streams_of[0], (3, NLON, NLAT), 1.0, 6.0, ((1, 32), (2, 2)), jnp.float32),
        "stress_start": scatter_about(streams_of[1], (3, NLON, NLAT), 0.5, 3.0, ((1, 32), (2, 2)), jnp.float32),
        "concentration": jnp.clip(0.5 + 0.5 * jax.random.uniform(streams_of[2], (NLON, NLAT), jnp.float32) ** shard_levels(streams_of[2], (NLON, NLAT), ((0, 32), (1, 2)), -0.2, 0.2), 0.5, 1.0),
        "cell_class": set_ends(jax.random.randint(part_splits[3], (NLON, NLAT), 0, 8), jax.random.fold_in(part_splits[3], 1), 0, 7).astype(jnp.int32),
        "land_mask": set_ends((jax.random.randint(streams_of[4], (NLON, NLAT), 0, 4) < 3).astype(jnp.int32), jax.random.fold_in(streams_of[4], 1), 0, 1),
        "fold_partner": jax.random.permutation(streams_of[5], NLON).astype(jnp.int32),
        "kernel_weights": jnp.clip(jnp.exp(jax.random.uniform(streams_of[6], (KW, KW), jnp.float32, math.log(0.05), math.log(0.5))), 0.05, 0.5),
    }


def extend(fields, partner, width):
    top = fields[:, :, -width:]
    north = jnp.take(top, partner, axis=1)[:, :, ::-1]
    south = jnp.zeros_like(north)
    tall = jnp.concatenate([south, fields, north], axis=2)
    return jnp.concatenate([tall[:, -width:], tall, tall[:, :width]], axis=1)

def smooth(padded, weights, ncols, nrows):
    side = weights.shape[0]
    total = jnp.zeros((padded.shape[0], ncols, nrows), jnp.float32)
    for first in range(side):
        for second in range(side):
            total = total + weights[first, second] * padded[:, first:first + ncols, second:second + nrows]
    return total

def reference(strain_rate, stress_start, concentration, cell_class, land_mask, fold_partner, kernel_weights):
    width = kernel_weights.shape[0] // 2
    ocean = land_mask.astype(jnp.float32)
    ncols, nrows = ocean.shape
    denom = smooth(extend(ocean[None], fold_partner, width), kernel_weights, ncols, nrows)[0] + 1.0
    count = jnp.sum(ocean)
    damage = ocean * 0.1 * cell_class.astype(jnp.float32) * concentration
    stress = ocean[None] * stress_start
    base = concentration * jnp.exp(-2.0 * (1.0 - concentration))
    e_one, e_two, e_shear = (strain_rate[0], strain_rate[1], strain_rate[2])
    load = jnp.stack([e_one + e_two / 3.0, e_two + e_one / 3.0, e_shear / (4.0 / 3.0)]) / (8.0 / 9.0)
    means = []
    for step in range(ITERS):
        keep = 1.0 - damage
        theta = 0.5 / (keep * keep)
        elastic = ocean[None] * (stress + (base * keep)[None] * load) / (1.0 + theta)[None]
        half_diff = (elastic[0] - elastic[1]) / 2.0
        tau = jnp.sqrt(half_diff * half_diff + elastic[2] * elastic[2] + 0.25)
        ratio = (tau + 0.7 * (elastic[0] + elastic[1]) / 2.0) / (0.6 * concentration)
        over = jnp.maximum(ratio, 1.0)
        q_part = 1.0 - 1.0 / over
        mean_now = jnp.sum(ocean * (over - 1.0)) / (count + 1.0)
        means.append(mean_now)
        factor = 1.0 / (1.0 + 2.0 * mean_now)
        local_damage = ocean * (damage + factor * keep * q_part)
        local_stress = elastic * (1.0 - factor * q_part)[None]
        fields = jnp.concatenate([local_damage[None], local_stress], axis=0)
        averaged = smooth(extend(fields, fold_partner, width), kernel_weights, ncols, nrows) / denom[None]
        fresh = ocean[None] * (0.5 * fields + 0.5 * averaged)
        damage = fresh[0]
        stress = fresh[1:]
    return (stress, damage, jnp.stack(means).astype(jnp.float32))
```

```python
import functools
import jax
import jax.numpy as jnp
from jax import lax
from jax.experimental import pallas as pl
from jax.experimental.pallas import tpu as pltpu
from jax.sharding import PartitionSpec as P

ITERS = 3
HALO = 9
LANES = 128
PAD = 16
F32 = jnp.float32
VM = pl.BlockSpec(memory_space=pltpu.VMEM)
SM = pl.BlockSpec(memory_space=pltpu.SMEM)


def cost(flops, size):
    return pl.CostEstimate(flops=flops, bytes_accessed=size, transcendentals=0)


def physics(damage, stress, bl, rc, oc):
    keep = 1.0 - damage
    k2 = keep * keep
    g = oc * (k2 / (k2 + 0.5))
    e = [g * (stress[k] + keep * bl[k]) for k in range(3)]
    half = (e[0] - e[1]) * 0.5
    tau = jnp.sqrt(half * half + e[2] * e[2] + 0.25)
    over = jnp.maximum((tau + 0.35 * (e[0] + e[1])) * rc, 1.0)
    q = oc * (1.0 - 1.0 / over)
    return e, q, oc * (over - 1.0)


def tops(tiles, single, extra, at):
    t = jnp.concatenate(tiles, axis=0).T
    rows = [t[at - k : at - k + 1, :] for k in range(3)]
    for one in (single, extra):
        if one is not None:
            parts = [one] + [pltpu.roll(one, k, 1) for k in (1, 2)] + [jnp.zeros_like(one)]
            rows.append(jnp.concatenate(parts, axis=0).T[at : at + 1, :])
    return rows


def total(x):
    return jnp.sum(jnp.sum(x, axis=0, keepdims=True), axis=1, keepdims=True)


def first_kernel(nrows, lat_ref, strain, stress, conc, cls, mask, f_ref, lat_out, chunk_ref, sum_ref):
    nt = f_ref.shape[1]
    ncols = conc.shape[0]
    excess = jnp.zeros((ncols, LANES), F32)
    count = jnp.zeros((ncols, LANES), F32)
    last = {}
    lane = lax.broadcasted_iota(jnp.int32, (ncols, LANES), 1)
    f_ref[:, nt - 1] = jnp.zeros((8, ncols, LANES), F32)
    for c in range(nt):
        w = min(LANES, nrows - c * LANES)
        sl = slice(c * LANES, c * LANES + w)
        con = conc[:, sl]
        base = con * jnp.exp(-2.0 * (1.0 - con))
        oc = mask[:, sl].astype(F32)
        e1, e2, e3 = (strain[k, :, sl] for k in range(3))
        third = 1.0 / 3.0
        bl = [base * ((e1 + e2 * third) * 1.125), base * ((e2 + e1 * third) * 1.125), base * (e3 * (0.75 * 1.125))]
        st = [oc * stress[k, :, sl] for k in range(3)]
        d = oc * 0.1 * cls[:, sl].astype(F32) * con
        for k in range(3):
            f_ref[k, c, :, 0:w] = bl[k]
            f_ref[3 + k, c, :, 0:w] = st[k]
        f_ref[6, c, :, 0:w] = oc * con
        f_ref[7, c, :, 0:w] = d
    for c in range(nt):
        bl = [f_ref[k, c] for k in range(3)]
        st = [f_ref[3 + k, c] for k in range(3)]
        mc = f_ref[6, c]
        d = f_ref[7, c]
        oc = jnp.where(mc > 0.0, 1.0, 0.0)
        rc = 1.0 / (0.6 * jnp.where(mc > 0.0, mc, 1.0))
        e, q, over = physics(d, st, bl, rc, oc)
        excess = excess + over
        count = count + oc
    at = nrows - 1 - (nt - 1) * LANES
    rows = tops([d, q, e[0], e[1]], e[2], oc, at)
    s = total(excess)
    n = total(count)
    lane1 = lax.broadcasted_iota(jnp.int32, (1, LANES), 1)
    sums = jnp.where(lane1 == 96, s, 0.0) + jnp.where(lane1 == 97, n, 0.0)
    for k, row in enumerate(rows):
        chunk_ref[k : k + 1, :] = row
    sum_ref[...] = jnp.broadcast_to(sums, sum_ref.shape)
    north = lat_ref[0] == lat_ref[1]
    for f in range(8):
        lat_out[f] = jnp.where(north, f_ref[f, 0], f_ref[f, nt - 1])


def second_kernel(nrows, lat_ref, f_ref, lat_in, chunk_ref, sum_ref, sum_in, t8_ref, low_ref, high_ref, send_ref):
    nt = f_ref.shape[1]
    ncols = f_ref.shape[2]
    edge = nrows - (nt - 1) * LANES
    lane = lax.broadcasted_iota(jnp.int32, (ncols, LANES), 1)
    north = lat_ref[0] == lat_ref[1]
    own = lane < edge
    keep = jnp.where(north, (lane >= LANES - HALO).astype(jnp.int32), ((lane >= edge) & (lane < edge + HALO)).astype(jnp.int32)) > 0
    for f in range(8):
        got = jnp.where(north, pltpu.roll(lat_in[f], (LANES - edge) % LANES, 1), pltpu.roll(lat_in[f], edge, 1))
        t8_ref[f] = jnp.where(own, f_ref[f, nt - 1], jnp.where(keep, got, 0.0))
    for f in range(8):
        for c in range(nt):
            at = t8_ref.at[f] if c == nt - 1 else f_ref.at[f, c]
            low_ref[f, c] = at[0:8]
            low_ref[8, c, f : f + 1] = at[8:9]
            high_ref[f, c] = at[ncols - 8 : ncols]
            high_ref[8, c, f : f + 1] = at[ncols - 9 : ncols - 8]
    s = sum_ref[0:1, :] + sum_in[0:1, :]
    chunk = [chunk_ref[k : k + 1, :] for k in range(5)]
    chunk[3] = chunk[3] + s
    block = jnp.concatenate(chunk, axis=0)
    for n in range(send_ref.shape[0]):
        send_ref[n] = block


def ghosts(got_ref, sel_ref, col_ref, per, fields):
    n = got_ref.shape[0] // per
    parts = []
    for r in range(per):
        m = got_ref[pl.ds(r, n, stride=per), :]
        h = m.astype(jnp.bfloat16)
        m = m - h.astype(F32)
        h2 = m.astype(jnp.bfloat16)
        h3 = (m - h2.astype(F32)).astype(jnp.bfloat16)
        parts.append(jnp.concatenate([h, h2, h3], axis=0))
    picked = jnp.dot(sel_ref[...], jnp.concatenate(parts, axis=1), preferred_element_type=F32)
    lane = lax.broadcasted_iota(jnp.int32, (sel_ref.shape[0], LANES), 1)
    col = col_ref[...] == (lane & 31)
    group = lane >> 5
    picked = [jnp.where(col, picked[:, r * LANES : (r + 1) * LANES], 0.0) for r in range(per)]
    out = []
    for f in range(fields):
        vals = []
        for k in range(3):
            row, g = (k, f) if f < 4 else (3 + f - 4, k)
            vals.append(jnp.sum(jnp.where(group == g, picked[row], 0.0), axis=1, keepdims=True))
        out.append(vals)
    return out


def smooth_into(w_ref, g_ref, acc_ref, nf, lo, hi):
    nt = g_ref.shape[1]
    lane = lax.broadcasted_iota(jnp.int32, (8, LANES), 1)

    def body(step, _):
        f = step // (hi - lo)
        row = (lo + step % (hi - lo)) * 8
        mid, rolled, out = {}, {}, {}
        for c in range(nt):
            x = [g_ref[f, c, pl.ds(row + a - 3, 8), :] for a in range(7)]
            for b in range(7):
                t = w_ref[0, b] * x[0]
                for a in range(1, 7):
                    t = t + w_ref[a, b] * x[a]
                if b == 3:
                    mid[c] = t
                else:
                    rolled[c, b] = pltpu.roll(t, (3 - b) % LANES, 1)
        for c in range(nt):
            t = mid[c]
            for b in range(3):
                t = t + jnp.where(lane < 3 - b, rolled[(c - 1) % nt, b], rolled[c, b])
            for b in range(4, 7):
                t = t + jnp.where(lane >= LANES - (b - 3), rolled[(c + 1) % nt, b], rolled[c, b])
            acc_ref[f, c, pl.ds(pl.multiple_of(row, 8), 8), :] = t
        return 0

    lax.fori_loop(0, nf * (hi - lo), body, 0)


def put_ghosts(lat_ref, g_ref, gh, factor, nrows, row0, nrow, with_ocean):
    nt = g_ref.shape[1]
    edge = nrows - (nt - 1) * LANES
    lane = lax.broadcasted_iota(jnp.int32, (nrow, LANES), 1)
    north = (lat_ref[0] == lat_ref[1]).astype(jnp.int32)
    vals = []
    d, q = gh[0], gh[1]
    vals.append([d[k] + factor * (1.0 - d[k]) * q[k] for k in range(3)])
    for m in range(3):
        vals.append([gh[2 + m][k] * (1.0 - factor * q[k]) for k in range(3)])
    if with_ocean:
        vals.append(gh[5])
    for f, v in enumerate(vals):
        t = g_ref[f, nt - 1, row0 : row0 + nrow, :]
        for k in range(3):
            t = jnp.where(lane == jnp.where(north > 0, edge + k, -1), v[k][0:nrow], t)
        g_ref[f, nt - 1, row0 : row0 + nrow, :] = t


def step_sums(chunk_ref, sum_ref, rows, excess):
    s = total(excess)
    lane1 = lax.broadcasted_iota(jnp.int32, (1, LANES), 1)
    sums = jnp.where(lane1 == 96, s, 0.0)
    rows[3] = rows[3] + sums
    for k, row in enumerate(rows):
        chunk_ref[k : k + 1, :] = row
    zero = jnp.zeros((1, LANES), F32)
    for k in range(4):
        sum_ref[k : k + 1, :] = sums if k == 3 else zero


def lane_value(row, at):
    lane1 = lax.broadcasted_iota(jnp.int32, row.shape, 1)
    return jnp.sum(jnp.where(lane1 == at, row, 0.0), axis=1, keepdims=True)


def finish(nrows, ncols, g_ref, acc_ref, stat_in, dyn_ref, chunk_ref, sum_ref, lo, hi):
    nt = g_ref.shape[1]
    edge = nrows - (nt - 1) * LANES
    lane = lax.broadcasted_iota(jnp.int32, (8, LANES), 1)
    excess = jnp.zeros((8, LANES), F32)
    for c in range(nt):

        def body(i, excess):
            at = pl.ds(pl.multiple_of(i * 8, 8), 8)
            to = pl.ds(pl.multiple_of((i - lo) * 8, 8), 8)
            bl, rc, r = stat_in(c, at, to)
            new = [0.5 * g_ref[f, c, at, :] + r * acc_ref[f, c, at, :] for f in range(4)]
            oc = jnp.where(r > 0.0, 1.0, 0.0)
            e, q, over = physics(new[0], new[1:], bl, rc, oc)
            dyn_ref[0, c, to, :] = new[0]
            dyn_ref[1, c, to, :] = q
            for k in range(3):
                dyn_ref[2 + k, c, to, :] = e[k]
            mine = jnp.where((i >= PAD // 8) & (i < (PAD + ncols) // 8), over, 0.0)
            if c == nt - 1:
                mine = jnp.where(lane < edge, mine, 0.0)
            return excess + mine

        excess = lax.fori_loop(lo, hi, body, excess)
    own = slice(PAD - lo * 8, PAD - lo * 8 + ncols)
    tile = [dyn_ref[f, nt - 1, own, :] for f in range(5)]
    rows = tops(tile[:4], tile[4], None, edge - 1)
    step_sums(chunk_ref, sum_ref, rows, excess)


def third_kernel(
    nrows, lat_ref, w_ref, f_ref, t8_ref, low_in, high_in, got_ref, sel_ref, col_ref,
    dyn_ref, stat_ref, chunk_ref, sum_ref, mean_ref, g_ref, acc_ref, rc_ref,
):
    nt = f_ref.shape[1]
    ncols = f_ref.shape[2]
    rows = g_ref.shape[2]
    n = got_ref.shape[0] // 5
    sums = jnp.sum(got_ref[pl.ds(3, n, stride=5), :], axis=0, keepdims=True)
    count = lane_value(sums, 97) + 1.0
    mean = lane_value(sums, 96) / count
    factor = 1.0 / (1.0 + 2.0 * mean)
    lane1 = lax.broadcasted_iota(jnp.int32, (1, LANES), 1)
    mean_ref[...] = jnp.broadcast_to(jnp.where(lane1 == 0, mean, count), mean_ref.shape)
    factor8 = jnp.broadcast_to(factor, (8, LANES))
    lo, hi = 1, rows // 8 - 1
    for c in range(nt):

        def local(vals, row, nr, c=c):
            bl, st, mc, d = vals[0:3], vals[3:6], vals[6], vals[7]
            oc = jnp.where(mc > 0.0, 1.0, 0.0)
            rc = 1.0 / (0.6 * jnp.where(mc > 0.0, mc, 1.0))
            e, q, _ = physics(d, st, bl, rc, oc)
            f8 = factor8[0:nr]
            at = slice(row, row + nr)
            g_ref[0, c, at, :] = d + f8 * (1.0 - d) * q
            for k in range(3):
                g_ref[1 + k, c, at, :] = e[k] * (1.0 - f8 * q)
            g_ref[4, c, at, :] = oc
            if nr == 8:
                stat = slice(row - lo * 8, row - lo * 8 + 8)
                for k in range(3):
                    stat_ref[k, c, stat, :] = bl[k]
                stat_ref[3, c, stat, :] = rc

        local([high_in[8, c, f : f + 1, :] for f in range(8)], PAD - 9, 1)
        local([high_in[f, c] for f in range(8)], PAD - 8, 8)
        for i in range(ncols // 8):
            local([(t8_ref[f, 8 * i : 8 * i + 8, :] if c == nt - 1 else f_ref[f, c, 8 * i : 8 * i + 8, :]) for f in range(8)], PAD + 8 * i, 8)
        local([low_in[f, c] for f in range(8)], PAD + ncols, 8)
        local([low_in[8, c, f : f + 1, :] for f in range(8)], PAD + ncols + 8, 1)
    gh = ghosts(got_ref, sel_ref, col_ref, 5, 6)
    for i in range(lo, hi):
        stat_ref[4, nt - 1, 8 * (i - lo) : 8 * (i - lo) + 8, :] = g_ref[4, nt - 1, 8 * i : 8 * i + 8, :]
    put_ghosts(lat_ref, g_ref, gh, factor, nrows, 0, rows, True)
    smooth_into(w_ref, g_ref, acc_ref, 5, lo, hi)

    def stat_in(c, at, to):
        oc = stat_ref[4, c, to, :] if c == nt - 1 else g_ref[4, c, at, :]
        r = 0.5 * oc / (acc_ref[4, c, at, :] + 1.0)
        stat_ref[4, c, to, :] = r
        return [stat_ref[k, c, to, :] for k in range(3)], stat_ref[3, c, to, :], r

    finish(nrows, ncols, g_ref, acc_ref, stat_in, dyn_ref, chunk_ref, sum_ref, lo, hi)


def load_local(nrows, lat_ref, dyn_in, got_ref, sel_ref, col_ref, mean_in, mean_ref, g_ref):
    nt = g_ref.shape[1]
    n = got_ref.shape[0] // 4
    sums = jnp.sum(got_ref[pl.ds(3, n, stride=4), :], axis=0, keepdims=True)
    count = lane_value(mean_in[0:1, :], 1)
    mean = lane_value(sums, 96) / count
    factor = 1.0 / (1.0 + 2.0 * mean)
    lane1 = lax.broadcasted_iota(jnp.int32, (1, LANES), 1)
    mean_ref[...] = jnp.broadcast_to(jnp.where(lane1 == 0, mean, count), mean_ref.shape)
    f8 = jnp.broadcast_to(factor, (8, LANES))
    for c in range(nt):

        def body(i, _, c=c):
            fr = pl.ds(pl.multiple_of(i * 8, 8), 8)
            to = pl.ds(pl.multiple_of(i * 8 + 8, 8), 8)
            d, q = dyn_in[0, c, fr, :], dyn_in[1, c, fr, :]
            g_ref[0, c, to, :] = d + f8 * (1.0 - d) * q
            down = 1.0 - f8 * q
            for k in range(3):
                g_ref[1 + k, c, to, :] = dyn_in[2 + k, c, fr, :] * down
            return 0

        lax.fori_loop(0, dyn_in.shape[2] // 8, body, 0)
    gh = ghosts(got_ref, sel_ref, col_ref, 4, 5)
    put_ghosts(lat_ref, g_ref, gh, factor, nrows, 0, g_ref.shape[2], False)


def fourth_kernel(
    nrows, ncols, lat_ref, w_ref, dyn_in, stat_in_ref, got_ref, sel_ref, col_ref, mean_in,
    dyn_ref, chunk_ref, sum_ref, mean_ref, g_ref, acc_ref,
):
    load_local(nrows, lat_ref, dyn_in, got_ref, sel_ref, col_ref, mean_in, mean_ref, g_ref)
    lo, hi = 1, g_ref.shape[2] // 8 - 1
    smooth_into(w_ref, g_ref, acc_ref, 4, lo, hi)

    def stat_in(c, at, to):
        return [stat_in_ref[k, c, to, :] for k in range(3)], stat_in_ref[3, c, to, :], stat_in_ref[4, c, to, :]

    finish(nrows, ncols, g_ref, acc_ref, stat_in, dyn_ref, chunk_ref, sum_ref, lo, hi)


def fifth_kernel(
    nrows, ncols, lat_ref, w_ref, dyn_in, stat_in_ref, got_ref, sel_ref, col_ref, mean_in,
    stress_ref, damage_ref, mean_ref, g_ref, acc_ref,
):
    load_local(nrows, lat_ref, dyn_in, got_ref, sel_ref, col_ref, mean_in, mean_ref, g_ref)
    nt = g_ref.shape[1]
    smooth_into(w_ref, g_ref, acc_ref, 4, PAD // 8, (PAD + ncols) // 8)
    for c in range(nt):
        w = min(LANES, nrows - c * LANES)
        for i in range(ncols // 8):
            at = slice(PAD + 8 * i, PAD + 8 * i + 8)
            r = stat_in_ref[4, c, PAD - 8 + 8 * i : PAD + 8 * i, :]
            for f in range(4):
                v = (0.5 * g_ref[f, c, at, :] + r * acc_ref[f, c, at, :])[:, 0:w]
                if f == 0:
                    damage_ref[8 * i : 8 * i + 8, c * LANES : c * LANES + w] = v
                else:
                    stress_ref[f - 1, 8 * i : 8 * i + 8, c * LANES : c * LANES + w] = v


def shards(strain_rate, stress_start, concentration, cell_class, land_mask, fold_partner, kernel_weights):
    ncols, nrows = concentration.shape
    nt = -(-nrows // LANES)
    nlon = lax.axis_size("lon")
    nlat = lax.axis_size("lat")
    rows = ncols + 2 * PAD
    mid = rows - 16
    sds = lambda *s: jax.ShapeDtypeStruct(s, F32)
    lat = jnp.stack([lax.axis_index("lat"), jnp.int32(nlat - 1)]).astype(jnp.int32)

    columns = (lax.axis_index("lon") * ncols - PAD + jnp.arange(rows, dtype=jnp.int32)) % (ncols * nlon)
    partner = jnp.take(fold_partner, columns)
    sel = (partner[:, None] // ncols == jnp.arange(nlon)[None, :]).astype(jnp.bfloat16)
    sel = jnp.concatenate([sel, sel, sel], axis=1)
    col = jnp.broadcast_to((partner % ncols)[:, None], (rows, LANES)).astype(jnp.int32)

    f, lat_out, chunk, sums = pl.pallas_call(
        functools.partial(first_kernel, nrows),
        out_shape=(sds(8, nt, ncols, LANES), sds(8, ncols, LANES), sds(5, LANES), sds(8, LANES)),
        in_specs=[SM] + [VM] * 5, out_specs=(VM,) * 4, cost_estimate=cost(4000000, 2000000), name="first",
    )(lat, strain_rate, stress_start, concentration, cell_class, land_mask)
    swap = [(i, nlat - 1 - i) for i in range(nlat)]
    lat_in = lax.ppermute(lat_out, "lat", swap)
    sum_in = lax.ppermute(sums, "lat", swap)
    t8, low, high, send = pl.pallas_call(
        functools.partial(second_kernel, nrows),
        out_shape=(sds(8, ncols, LANES), sds(9, nt, 8, LANES), sds(9, nt, 8, LANES), sds(nlon, 5, LANES)),
        in_specs=[SM] + [VM] * 5, out_specs=(VM,) * 4, cost_estimate=cost(400000, 2000000), name="second",
    )(lat, f, lat_in, chunk, sums, sum_in)
    up = [(i, (i + 1) % nlon) for i in range(nlon)]
    down = [(j, i) for i, j in up]
    high_in = lax.ppermute(high, "lon", up)
    low_in = lax.ppermute(low, "lon", down)
    got = lax.all_to_all(send, "lon", 0, 0, tiled=True).reshape(nlon * 5, LANES)

    scratch = lambda nf: [pltpu.VMEM((nf, nt, rows, LANES), F32), pltpu.VMEM((nf, nt, rows, LANES), F32)]
    dyn, stat, chunk, sums, mean = pl.pallas_call(
        functools.partial(third_kernel, nrows),
        out_shape=(sds(5, nt, mid, LANES), sds(5, nt, mid, LANES), sds(4, LANES), sds(4, LANES), sds(8, LANES)),
        in_specs=[SM, SM] + [VM] * 7, out_specs=(VM,) * 5, scratch_shapes=scratch(5) + [pltpu.VMEM((8, LANES), F32)],
        cost_estimate=cost(40000000, 4000000), name="third",
    )(lat, kernel_weights, f, t8, low_in, high_in, got, sel, col)
    means = [mean[0, 0]]

    def spread(chunk, sums):
        chunk = chunk + lax.ppermute(sums, "lat", swap)
        send = jnp.broadcast_to(chunk[None], (nlon, 4, LANES))
        return lax.all_to_all(send, "lon", 0, 0, tiled=True).reshape(nlon * 4, LANES)

    got = spread(chunk, sums)
    dyn, chunk, sums, mean = pl.pallas_call(
        functools.partial(fourth_kernel, nrows, ncols),
        out_shape=(sds(5, nt, mid, LANES), sds(4, LANES), sds(4, LANES), sds(8, LANES)),
        in_specs=[SM, SM] + [VM] * 6, out_specs=(VM,) * 4, scratch_shapes=scratch(4),
        cost_estimate=cost(30000000, 4000000), name="fourth",
    )(lat, kernel_weights, dyn, stat, got, sel, col, mean)
    means.append(mean[0, 0])
    got = spread(chunk, sums)
    stress, damage, mean = pl.pallas_call(
        functools.partial(fifth_kernel, nrows, ncols),
        out_shape=(sds(3, ncols, nrows), sds(ncols, nrows), sds(8, LANES)),
        in_specs=[SM, SM] + [VM] * 6, out_specs=(VM,) * 3, scratch_shapes=scratch(4),
        cost_estimate=cost(20000000, 4000000), name="fifth",
    )(lat, kernel_weights, dyn, stat, got, sel, col, mean)
    means.append(mean[0, 0])
    return stress, damage, jnp.stack(means)


def solution(mesh):
    in_specs = (
        P(None, "lon", "lat"),
        P(None, "lon", "lat"),
        P("lon", "lat"),
        P(("member", "lon"), "lat"),
        P("lon", "lat"),
        P(),
        P(),
    )
    out_specs = (P(None, ("member", "lon"), "lat"), P(("member", "lon"), "lat"), P("member"))
    return jax.shard_map(shards, mesh=mesh, in_specs=in_specs, out_specs=out_specs, check_vma=False)
```

```python
import functools
import jax
import jax.numpy as jnp
from jax import lax
from jax.experimental import pallas as pl
from jax.experimental.pallas import tpu as pltpu
from jax.sharding import PartitionSpec as P


ITERS = 3
HALO = 9
LANES = 128
PAD = 16
F32 = jnp.float32
VM = pl.BlockSpec(memory_space=pltpu.VMEM)
SM = pl.BlockSpec(memory_space=pltpu.SMEM)


def small():
    return pltpu.CompilerParams(vmem_limit_bytes=12 * 1024 * 1024)


def is_north():
    return lax.axis_index("lat") == lax.axis_size("lat") - 1


def cost(flops, size):
    return pl.CostEstimate(flops=flops, bytes_accessed=size, transcendentals=0)


def overstress(e, rc):
    half = (e[0] - e[1]) * 0.5
    tau = jnp.sqrt(half * half + e[2] * e[2] + 0.25)
    over = jnp.maximum((tau + 0.35 * (e[0] + e[1])) * rc, 1.0)
    return over - 1.0, 1.0 - 1.0 / over


def physics(damage, stress, bl, rc, oc):
    keep = 1.0 - damage
    k2 = keep * keep
    g = oc * (k2 / (k2 + 0.5))
    e = [g * (stress[k] + keep * bl[k]) for k in range(3)]
    excess, q = overstress(e, rc)
    return e, oc * q, oc * excess


def tops(tiles, single, at):
    t = jnp.concatenate(tiles, axis=0).T
    rows = [t[at - k : at - k + 1, :] for k in range(3)]
    parts = [single] + [pltpu.roll(single, k, 1) for k in (1, 2)] + [jnp.zeros_like(single)]
    return rows + [jnp.concatenate(parts, axis=0).T[at : at + 1, :]]


def total(x):
    return jnp.sum(jnp.sum(x, axis=0, keepdims=True), axis=1, keepdims=True)


def first_kernel(nrows, *refs):
    given, (f_ref, lat_out, chunk_ref, sum_ref), held, sem = refs[:5], refs[5:9], refs[9:14], refs[14]
    copies = [pltpu.make_async_copy(a, b, sem.at[n]) for n, (a, b) in enumerate(zip(given, held, strict=True))]
    for copy in copies:
        copy.start()
    for copy in copies:
        copy.wait()
    strain, stress, conc, cls, mask = held
    nt = f_ref.shape[1]
    ncols = conc.shape[0]
    excess = jnp.zeros((ncols, LANES), F32)
    count = jnp.zeros((ncols, LANES), F32)
    lane = lax.broadcasted_iota(jnp.int32, (ncols, LANES), 1)
    f_ref[:, nt - 1] = jnp.zeros((8, ncols, LANES), F32)
    for c in range(nt):
        w = min(LANES, nrows - c * LANES)
        sl = slice(c * LANES, c * LANES + w)
        con = conc[:, sl]
        base = con * jnp.exp(-2.0 * (1.0 - con))
        oc = mask[:, sl].astype(F32)
        e1, e2, e3 = (strain[k, :, sl] for k in range(3))
        third = 1.0 / 3.0
        bl = [base * ((e1 + e2 * third) * 1.125), base * ((e2 + e1 * third) * 1.125), base * (e3 * (0.75 * 1.125))]
        st = [oc * stress[k, :, sl] for k in range(3)]
        d = oc * 0.1 * cls[:, sl].astype(F32) * con
        for k in range(3):
            f_ref[k, c, :, 0:w] = bl[k]
            f_ref[3 + k, c, :, 0:w] = st[k]
        f_ref[6, c, :, 0:w] = oc * con
        f_ref[7, c, :, 0:w] = d
    for c in range(nt):
        bl = [f_ref[k, c] for k in range(3)]
        st = [f_ref[3 + k, c] for k in range(3)]
        mc = f_ref[6, c]
        d = f_ref[7, c]
        oc = jnp.where(mc > 0.0, 1.0, 0.0)
        rc = 1.0 / (0.6 * jnp.where(mc > 0.0, mc, 1.0))
        e, _, over = physics(d, st, bl, rc, oc)
        excess = excess + over
        count = count + oc
    at = nrows - 1 - (nt - 1) * LANES
    rows = tops([d, mc, e[0], e[1]], e[2], at)
    s = total(excess)
    n = total(count)
    lane1 = lax.broadcasted_iota(jnp.int32, (1, LANES), 1)
    sums = jnp.where(lane1 == 96, s, 0.0) + jnp.where(lane1 == 97, n, 0.0)
    for k, row in enumerate(rows):
        chunk_ref[k : k + 1, :] = row
    sum_ref[...] = jnp.broadcast_to(sums, sum_ref.shape)
    north = is_north()
    for f in range(8):
        lat_out[f] = jnp.where(north, f_ref[f, 0], f_ref[f, nt - 1])


def second_kernel(nrows, f_ref, lat_in, chunk_ref, sum_ref, sum_in, t8_ref, low_ref, high_ref, send_ref):
    nt = f_ref.shape[1]
    ncols = f_ref.shape[2]
    edge = nrows - (nt - 1) * LANES
    lane = lax.broadcasted_iota(jnp.int32, (ncols, LANES), 1)
    north = is_north()
    own = lane < edge
    keep = jnp.where(north, (lane >= LANES - HALO).astype(jnp.int32), ((lane >= edge) & (lane < edge + HALO)).astype(jnp.int32)) > 0
    for f in range(8):
        got = jnp.where(north, pltpu.roll(lat_in[f], (LANES - edge) % LANES, 1), pltpu.roll(lat_in[f], edge, 1))
        t8_ref[f] = jnp.where(own, f_ref[f, nt - 1], jnp.where(keep, got, 0.0))
    for f in range(8):
        for c in range(nt):
            at = t8_ref.at[f] if c == nt - 1 else f_ref.at[f, c]
            low_ref[f, c] = at[0:8]
            low_ref[8, c, f : f + 1] = at[8:9]
            high_ref[f, c] = at[ncols - 8 : ncols]
            high_ref[8, c, f : f + 1] = at[ncols - 9 : ncols - 8]
    s = sum_ref[0:1, :] + sum_in[0:1, :]
    chunk = [chunk_ref[k : k + 1, :] for k in range(4)]
    chunk[3] = chunk[3] + s
    block = jnp.concatenate(chunk, axis=0)
    for n in range(send_ref.shape[0]):
        send_ref[n] = block


def ghosts(got_ref, sel_ref, col_ref):
    n = got_ref.shape[0] // 4
    parts = []
    for r in range(4):
        m = got_ref[pl.ds(r, n, stride=4), :]
        h = m.astype(jnp.bfloat16)
        m = m - h.astype(F32)
        h2 = m.astype(jnp.bfloat16)
        h3 = (m - h2.astype(F32)).astype(jnp.bfloat16)
        parts.append(jnp.concatenate([h, h2, h3], axis=0))
    picked = jnp.dot(sel_ref[...], jnp.concatenate(parts, axis=1), preferred_element_type=F32)
    lane = lax.broadcasted_iota(jnp.int32, (sel_ref.shape[0], LANES), 1)
    col = col_ref[...] == (lane & 31)
    group = lane >> 5
    picked = [jnp.where(col, picked[:, r * LANES : (r + 1) * LANES], 0.0) for r in range(4)]
    out = []
    for f in range(5):
        vals = []
        for k in range(3):
            row, g = (k, f) if f < 4 else (3, k)
            vals.append(jnp.sum(jnp.where(group == g, picked[row], 0.0), axis=1, keepdims=True))
        out.append(vals)
    return out


def smooth_into(w_ref, g_ref, acc_ref, nf, lo, hi):
    nt = g_ref.shape[1]
    lane = lax.broadcasted_iota(jnp.int32, (8, LANES), 1)

    def body(step, _):
        f = step // (hi - lo)
        row = (lo + step % (hi - lo)) * 8
        mid, rolled = {}, {}
        for c in range(nt):
            x = [g_ref[f, c, pl.ds(row + a - 3, 8), :] for a in range(7)]
            for b in range(7):
                t = w_ref[0, b] * x[0]
                for a in range(1, 7):
                    t = t + w_ref[a, b] * x[a]
                if b == 3:
                    mid[c] = t
                else:
                    rolled[c, b] = pltpu.roll(t, (3 - b) % LANES, 1)
        for c in range(nt):
            t = mid[c]
            for b in range(3):
                t = t + jnp.where(lane < 3 - b, rolled[(c - 1) % nt, b], rolled[c, b])
            for b in range(4, 7):
                t = t + jnp.where(lane >= LANES - (b - 3), rolled[(c + 1) % nt, b], rolled[c, b])
            acc_ref[f, c, pl.ds(pl.multiple_of(row, 8), 8), :] = t
        return 0

    lax.fori_loop(0, nf * (hi - lo), body, 0)


def put_ghosts(g_ref, gh, factor, nrows, row0, nrow, first):
    nt = g_ref.shape[1]
    edge = nrows - (nt - 1) * LANES
    lane = lax.broadcasted_iota(jnp.int32, (nrow, LANES), 1)
    north = is_north().astype(jnp.int32)
    vals = []
    d, q = gh[0], gh[1]
    if first:
        oc = [jnp.where(v > 0.0, 1.0, 0.0) for v in q]
        rc = [1.0 / (0.6 * jnp.where(v > 0.0, v, 1.0)) for v in q]
        q = [oc[k] * overstress([gh[2 + m][k] for m in range(3)], rc[k])[1] for k in range(3)]
    vals.append([d[k] + factor * (1.0 - d[k]) * q[k] for k in range(3)])
    for m in range(3):
        vals.append([gh[2 + m][k] * (1.0 - factor * q[k]) for k in range(3)])
    if first:
        vals.append(oc)
    for f, v in enumerate(vals):
        t = g_ref[f, nt - 1, row0 : row0 + nrow, :]
        for k in range(3):
            t = jnp.where(lane == jnp.where(north > 0, edge + k, -1), v[k][0:nrow], t)
        g_ref[f, nt - 1, row0 : row0 + nrow, :] = t


def step_sums(chunk_ref, sum_ref, rows, excess):
    s = total(excess)
    lane1 = lax.broadcasted_iota(jnp.int32, (1, LANES), 1)
    sums = jnp.where(lane1 == 96, s, 0.0)
    rows[3] = rows[3] + sums
    for k, row in enumerate(rows):
        chunk_ref[k : k + 1, :] = row
    zero = jnp.zeros((1, LANES), F32)
    for k in range(4):
        sum_ref[k : k + 1, :] = sums if k == 3 else zero


def lane_value(row, at):
    lane1 = lax.broadcasted_iota(jnp.int32, row.shape, 1)
    return jnp.sum(jnp.where(lane1 == at, row, 0.0), axis=1, keepdims=True)


def finish(nrows, ncols, g_ref, acc_ref, stat_in, dyn_ref, chunk_ref, sum_ref, lo, hi):
    nt = g_ref.shape[1]
    edge = nrows - (nt - 1) * LANES
    lane = lax.broadcasted_iota(jnp.int32, (8, LANES), 1)
    excess = jnp.zeros((8, LANES), F32)
    for c in range(nt):

        def body(i, excess):
            at = pl.ds(pl.multiple_of(i * 8, 8), 8)
            to = pl.ds(pl.multiple_of((i - lo) * 8, 8), 8)
            bl, rc, r = stat_in(c, at, to)
            new = [0.5 * g_ref[f, c, at, :] + r * acc_ref[f, c, at, :] for f in range(4)]
            oc = jnp.where(r > 0.0, 1.0, 0.0)
            e, q, over = physics(new[0], new[1:], bl, rc, oc)
            dyn_ref[0, c, to, :] = new[0]
            dyn_ref[1, c, to, :] = q
            for k in range(3):
                dyn_ref[2 + k, c, to, :] = e[k]
            mine = jnp.where((i >= PAD // 8) & (i < (PAD + ncols) // 8), over, 0.0)
            if c == nt - 1:
                mine = jnp.where(lane < edge, mine, 0.0)
            return excess + mine

        excess = lax.fori_loop(lo, hi, body, excess)
    own = slice(PAD - lo * 8, PAD - lo * 8 + ncols)
    tile = [dyn_ref[f, nt - 1, own, :] for f in range(5)]
    rows = tops(tile[:4], tile[4], edge - 1)
    step_sums(chunk_ref, sum_ref, rows, excess)


def third_kernel(
    nrows, w_ref, f_ref, t8_ref, low_in, high_in, got_ref, sel_ref, col_ref,
    dyn_ref, stat_ref, chunk_ref, sum_ref, mean_ref, g_ref, acc_ref, rc_ref,
):
    nt = f_ref.shape[1]
    ncols = f_ref.shape[2]
    rows = g_ref.shape[2]
    n = got_ref.shape[0] // 4
    sums = jnp.sum(got_ref[pl.ds(3, n, stride=4), :], axis=0, keepdims=True)
    count = lane_value(sums, 97) + 1.0
    mean = lane_value(sums, 96) / count
    factor = 1.0 / (1.0 + 2.0 * mean)
    lane1 = lax.broadcasted_iota(jnp.int32, (1, LANES), 1)
    mean_ref[...] = jnp.broadcast_to(jnp.where(lane1 == 1, mean, count), mean_ref.shape)
    factor8 = jnp.broadcast_to(factor, (8, LANES))
    lo, hi = 1, rows // 8 - 1
    for c in range(nt):

        def local(vals, row, nr, c=c):
            bl, st, mc, d = vals[0:3], vals[3:6], vals[6], vals[7]
            oc = jnp.where(mc > 0.0, 1.0, 0.0)
            rc = 1.0 / (0.6 * jnp.where(mc > 0.0, mc, 1.0))
            e, q, _ = physics(d, st, bl, rc, oc)
            f8 = factor8[0:nr]
            at = slice(row, row + nr)
            g_ref[0, c, at, :] = d + f8 * (1.0 - d) * q
            for k in range(3):
                g_ref[1 + k, c, at, :] = e[k] * (1.0 - f8 * q)
            g_ref[4, c, at, :] = oc
            if nr == 8:
                stat = slice(row - lo * 8, row - lo * 8 + 8)
                for k in range(3):
                    stat_ref[k, c, stat, :] = bl[k]
                stat_ref[3, c, stat, :] = rc

        local([high_in[8, c, f : f + 1, :] for f in range(8)], PAD - 9, 1)
        local([high_in[f, c] for f in range(8)], PAD - 8, 8)
        for i in range(ncols // 8):
            local([(t8_ref[f, 8 * i : 8 * i + 8, :] if c == nt - 1 else f_ref[f, c, 8 * i : 8 * i + 8, :]) for f in range(8)], PAD + 8 * i, 8)
        local([low_in[f, c] for f in range(8)], PAD + ncols, 8)
        local([low_in[8, c, f : f + 1, :] for f in range(8)], PAD + ncols + 8, 1)
    gh = ghosts(got_ref, sel_ref, col_ref)
    for i in range(lo, hi):
        stat_ref[4, nt - 1, 8 * (i - lo) : 8 * (i - lo) + 8, :] = g_ref[4, nt - 1, 8 * i : 8 * i + 8, :]
    put_ghosts(g_ref, gh, factor, nrows, 0, rows, True)
    smooth_into(w_ref, g_ref, acc_ref, 5, lo, hi)

    def stat_in(c, at, to):
        oc = stat_ref[4, c, to, :] if c == nt - 1 else g_ref[4, c, at, :]
        r = 0.5 * oc / (acc_ref[4, c, at, :] + 1.0)
        stat_ref[4, c, to, :] = r
        return [stat_ref[k, c, to, :] for k in range(3)], stat_ref[3, c, to, :], r

    finish(nrows, ncols, g_ref, acc_ref, stat_in, dyn_ref, chunk_ref, sum_ref, lo, hi)


def load_local(nrows, dyn_in, got_ref, sel_ref, col_ref, mean_in, g_ref):
    nt = g_ref.shape[1]
    n = got_ref.shape[0] // 4
    sums = jnp.sum(got_ref[pl.ds(3, n, stride=4), :], axis=0, keepdims=True)
    mean = lane_value(sums, 96) / lane_value(mean_in[0:1, :], 0)
    factor = 1.0 / (1.0 + 2.0 * mean)
    f8 = jnp.broadcast_to(factor, (8, LANES))
    for c in range(nt):

        def body(i, _, c=c):
            fr = pl.ds(pl.multiple_of(i * 8, 8), 8)
            to = pl.ds(pl.multiple_of(i * 8 + 8, 8), 8)
            d, q = dyn_in[0, c, fr, :], dyn_in[1, c, fr, :]
            g_ref[0, c, to, :] = d + f8 * (1.0 - d) * q
            down = 1.0 - f8 * q
            for k in range(3):
                g_ref[1 + k, c, to, :] = dyn_in[2 + k, c, fr, :] * down
            return 0

        lax.fori_loop(0, dyn_in.shape[2] // 8, body, 0)
    gh = ghosts(got_ref, sel_ref, col_ref)
    put_ghosts(g_ref, gh, factor, nrows, 0, g_ref.shape[2], False)
    return mean


def fourth_kernel(
    nrows, ncols, w_ref, dyn_in, stat_in_ref, got_ref, sel_ref, col_ref, mean_in,
    dyn_ref, chunk_ref, sum_ref, mean_ref, g_ref, acc_ref,
):
    mean = load_local(nrows, dyn_in, got_ref, sel_ref, col_ref, mean_in, g_ref)
    lane = lax.broadcasted_iota(jnp.int32, mean_ref.shape, 1)
    mean_ref[...] = jnp.where(lane == 2, mean, mean_in[...])
    lo, hi = 1, g_ref.shape[2] // 8 - 1
    smooth_into(w_ref, g_ref, acc_ref, 4, lo, hi)

    def stat_in(c, at, to):
        return [stat_in_ref[k, c, to, :] for k in range(3)], stat_in_ref[3, c, to, :], stat_in_ref[4, c, to, :]

    finish(nrows, ncols, g_ref, acc_ref, stat_in, dyn_ref, chunk_ref, sum_ref, lo, hi)


def fifth_kernel(
    nrows, ncols, w_ref, dyn_in, stat_in_ref, got_ref, sel_ref, col_ref, mean_in,
    stress_ref, damage_ref, mean_ref, g_ref, acc_ref,
):
    mean = load_local(nrows, dyn_in, got_ref, sel_ref, col_ref, mean_in, g_ref)
    row = mean_in[0:1, :]
    for at, one in enumerate((lane_value(row, 1), lane_value(row, 2), mean)):
        mean_ref[at] = jnp.sum(one)
    nt = g_ref.shape[1]
    smooth_into(w_ref, g_ref, acc_ref, 4, PAD // 8, (PAD + ncols) // 8)
    for c in range(nt):
        w = min(LANES, nrows - c * LANES)
        for i in range(ncols // 8):
            at = slice(PAD + 8 * i, PAD + 8 * i + 8)
            r = stat_in_ref[4, c, PAD - 8 + 8 * i : PAD + 8 * i, :]
            for f in range(4):
                v = (0.5 * g_ref[f, c, at, :] + r * acc_ref[f, c, at, :])[:, 0:w]
                if f == 0:
                    damage_ref[8 * i : 8 * i + 8, c * LANES : c * LANES + w] = v
                else:
                    stress_ref[f - 1, 8 * i : 8 * i + 8, c * LANES : c * LANES + w] = v


def shards(strain_rate, stress_start, concentration, cell_class, land_mask, fold_partner, kernel_weights):
    ncols, nrows = concentration.shape
    nt = -(-nrows // LANES)
    nlon = lax.axis_size("lon")
    nlat = lax.axis_size("lat")
    rows = ncols + 2 * PAD
    mid = rows - 16
    sds = lambda *s: jax.ShapeDtypeStruct(s, F32)

    columns = (lax.axis_index("lon") * ncols - PAD + jnp.arange(rows, dtype=jnp.int32)) % (ncols * nlon)
    partner = jnp.take(fold_partner, columns)
    sel = (partner[:, None] // ncols == jnp.arange(nlon)[None, :]).astype(jnp.bfloat16)
    sel = jnp.concatenate([sel, sel, sel], axis=1)
    col = jnp.broadcast_to((partner % ncols)[:, None], (rows, LANES)).astype(jnp.int32)

    given = (strain_rate, stress_start, concentration, cell_class, land_mask)
    f, lat_out, chunk, sums = pl.pallas_call(
        functools.partial(first_kernel, nrows),
        out_shape=(sds(8, nt, ncols, LANES), sds(8, ncols, LANES), sds(4, LANES), sds(8, LANES)),
        in_specs=[pl.BlockSpec(memory_space=pltpu.HBM)] * 5, out_specs=(VM,) * 4,
        scratch_shapes=[pltpu.VMEM(a.shape, a.dtype) for a in given] + [pltpu.SemaphoreType.DMA((5,))],
        cost_estimate=cost(4000000, 2000000), compiler_params=small(), name="first",
    )(*given)
    swap = [(i, nlat - 1 - i) for i in range(nlat)]
    lat_in = lax.ppermute(lat_out, "lat", swap)
    sum_in = lax.ppermute(sums, "lat", swap)
    t8, low, high, send = pl.pallas_call(
        functools.partial(second_kernel, nrows),
        out_shape=(sds(8, ncols, LANES), sds(9, nt, 8, LANES), sds(9, nt, 8, LANES), sds(nlon, 4, LANES)),
        in_specs=[VM] * 5, out_specs=(VM,) * 4, cost_estimate=cost(400000, 2000000), compiler_params=small(), name="second",
    )(f, lat_in, chunk, sums, sum_in)
    up = [(i, (i + 1) % nlon) for i in range(nlon)]
    down = [(j, i) for i, j in up]
    high_in = lax.ppermute(high, "lon", up)
    low_in = lax.ppermute(low, "lon", down)
    got = lax.all_to_all(send, "lon", 0, 0, tiled=True).reshape(nlon * 4, LANES)

    scratch = lambda nf: [pltpu.VMEM((nf, nt, rows, LANES), F32), pltpu.VMEM((nf, nt, rows, LANES), F32)]
    dyn, stat, chunk, sums, mean = pl.pallas_call(
        functools.partial(third_kernel, nrows),
        out_shape=(sds(5, nt, mid, LANES), sds(5, nt, mid, LANES), sds(4, LANES), sds(4, LANES), sds(8, LANES)),
        in_specs=[SM] + [VM] * 7, out_specs=(VM,) * 5, scratch_shapes=scratch(5) + [pltpu.VMEM((8, LANES), F32)],
        cost_estimate=cost(40000000, 4000000), compiler_params=small(), name="third",
    )(kernel_weights, f, t8, low_in, high_in, got, sel, col)

    def spread(chunk, sums):
        chunk = chunk + lax.ppermute(sums, "lat", swap)
        send = jnp.broadcast_to(chunk[None], (nlon, 4, LANES))
        return lax.all_to_all(send, "lon", 0, 0, tiled=True).reshape(nlon * 4, LANES)

    got = spread(chunk, sums)
    dyn, chunk, sums, mean = pl.pallas_call(
        functools.partial(fourth_kernel, nrows, ncols),
        out_shape=(sds(5, nt, mid, LANES), sds(4, LANES), sds(4, LANES), sds(8, LANES)),
        in_specs=[SM] + [VM] * 6, out_specs=(VM,) * 4, scratch_shapes=scratch(4),
        cost_estimate=cost(30000000, 4000000), compiler_params=small(), name="fourth",
    )(kernel_weights, dyn, stat, got, sel, col, mean)
    got = spread(chunk, sums)
    stress, damage, mean = pl.pallas_call(
        functools.partial(fifth_kernel, nrows, ncols),
        out_shape=(sds(3, ncols, nrows), sds(ncols, nrows), sds(ITERS)),
        in_specs=[SM] + [VM] * 6, out_specs=(VM, VM, SM), scratch_shapes=scratch(4),
        cost_estimate=cost(20000000, 4000000), compiler_params=small(), name="fifth",
    )(kernel_weights, dyn, stat, got, sel, col, mean)
    return stress, damage, mean


def solution(mesh):
    in_specs = (
        P(None, "lon", "lat"),
        P(None, "lon", "lat"),
        P("lon", "lat"),
        P(("member", "lon"), "lat"),
        P("lon", "lat"),
        P(),
        P(),
    )
    out_specs = (P(None, ("member", "lon"), "lat"), P(("member", "lon"), "lat"), P("member"))
    return jax.shard_map(shards, mesh=mesh, in_specs=in_specs, out_specs=out_specs, check_vma=False)
```

```python
import functools
import jax
import jax.numpy as jnp
from jax import lax
from jax.experimental import pallas as pl
from jax.experimental.pallas import tpu as pltpu
from jax.sharding import PartitionSpec as P


ITERS = 3
HALO = 9
LANES = 128
PAD = 16
F32 = jnp.float32
VM = pl.BlockSpec(memory_space=pltpu.VMEM)
SM = pl.BlockSpec(memory_space=pltpu.SMEM)


def small():
    return pltpu.CompilerParams(vmem_limit_bytes=12 * 1024 * 1024)


def is_north():
    return lax.axis_index("lat") == lax.axis_size("lat") - 1


def cost(flops, size):
    return pl.CostEstimate(flops=flops, bytes_accessed=size, transcendentals=0)


def overstress(e, rc):
    half = (e[0] - e[1]) * 0.5
    tau = jnp.sqrt(half * half + e[2] * e[2] + 0.25)
    over = jnp.maximum((tau + 0.35 * (e[0] + e[1])) * rc, 1.0)
    return over - 1.0, 1.0 - 1.0 / over


def physics(damage, stress, bl, rc):
    keep = 1.0 - damage
    k2 = keep * keep
    g = k2 / (k2 + 0.5)
    e = [g * (stress[k] + keep * bl[k]) for k in range(3)]
    excess, q = overstress(e, rc)
    return e, q, excess


def tops(tiles, single, at):
    t = jnp.concatenate(tiles, axis=0).T
    rows = [t[at - k : at - k + 1, :] for k in range(3)]
    parts = [single] + [pltpu.roll(single, k, 1) for k in (1, 2)] + [jnp.zeros_like(single)]
    return rows + [jnp.concatenate(parts, axis=0).T[at : at + 1, :]]


def total(x):
    return jnp.sum(jnp.sum(x, axis=0, keepdims=True), axis=1, keepdims=True)


def first_kernel(nrows, *refs):
    given, (f_ref, lat_out, chunk_ref, sum_ref), held, sem = refs[:5], refs[5:9], refs[9:14], refs[14]
    copies = [pltpu.make_async_copy(a, b, sem.at[n]) for n, (a, b) in enumerate(zip(given, held, strict=True))]
    for n in (2, 4, 3, 0, 1):
        copies[n].start()
    strain, stress, conc, cls, mask = held
    nt = f_ref.shape[1]
    ncols = conc.shape[0]
    f_ref[:, nt - 1] = jnp.zeros((8, ncols, LANES), F32)
    parts = [(c, min(LANES, nrows - c * LANES), slice(c * LANES, min(nrows, (c + 1) * LANES))) for c in range(nt)]
    for n in (2, 4, 3):
        copies[n].wait()
    for c, w, sl in parts:
        con = conc[:, sl]
        oc = mask[:, sl].astype(F32)
        f_ref[0, c, :, 0:w] = oc * con * jnp.exp(-2.0 * (1.0 - con))
        f_ref[6, c, :, 0:w] = oc * con
        f_ref[7, c, :, 0:w] = oc * 0.1 * cls[:, sl].astype(F32) * con
    copies[0].wait()
    third = 1.0 / 3.0
    for c, w, sl in parts:
        e1, e2, e3 = (strain[k, :, sl] for k in range(3))
        base = f_ref[0, c, :, 0:w]
        f_ref[0, c, :, 0:w] = base * ((e1 + e2 * third) * 1.125)
        f_ref[1, c, :, 0:w] = base * ((e2 + e1 * third) * 1.125)
        f_ref[2, c, :, 0:w] = base * (e3 * (0.75 * 1.125))
    copies[1].wait()
    for c, w, sl in parts:
        oc = jnp.where(f_ref[6, c, :, 0:w] > 0.0, 1.0, 0.0)
        for k in range(3):
            f_ref[3 + k, c, :, 0:w] = oc * stress[k, :, sl]
    excess = jnp.zeros((ncols, LANES), F32)
    count = jnp.zeros((ncols, LANES), F32)
    for c in range(nt):
        d, mc, e, _, over, oc, _ = start_state([f_ref[k, c] for k in range(8)])
        excess = excess + over
        count = count + oc
    at = nrows - 1 - (nt - 1) * LANES
    rows = tops([d, mc, e[0], e[1]], e[2], at)
    s = total(excess)
    n = total(count)
    lane1 = lax.broadcasted_iota(jnp.int32, (1, LANES), 1)
    sums = jnp.where(lane1 == 96, s, 0.0) + jnp.where(lane1 == 97, n, 0.0)
    for k, row in enumerate(rows):
        chunk_ref[k : k + 1, :] = row
    sum_ref[...] = jnp.broadcast_to(sums, sum_ref.shape)
    north = is_north()
    for f in range(8):
        lat_out[f] = jnp.where(north, f_ref[f, 0], f_ref[f, nt - 1])


def start_state(vals):
    bl, st, mc, d = vals[0:3], vals[3:6], vals[6], vals[7]
    oc = jnp.where(mc > 0.0, 1.0, 0.0)
    rc = oc / (0.6 * jnp.where(mc > 0.0, mc, 1.0))
    e, q, over = physics(d, st, bl, rc)
    return d, mc, e, q, over, oc, rc


def second_kernel(nrows, f_ref, lat_in, chunk_ref, sum_ref, sum_in, t8_ref, low_ref, high_ref, send_ref):
    nt = f_ref.shape[1]
    ncols = f_ref.shape[2]
    edge = nrows - (nt - 1) * LANES
    lane = lax.broadcasted_iota(jnp.int32, (ncols, LANES), 1)
    north = is_north()
    own = lane < edge
    keep = jnp.where(north, (lane >= LANES - HALO).astype(jnp.int32), ((lane >= edge) & (lane < edge + HALO)).astype(jnp.int32)) > 0
    for f in range(8):
        got = jnp.where(north, pltpu.roll(lat_in[f], (LANES - edge) % LANES, 1), pltpu.roll(lat_in[f], edge, 1))
        t8_ref[f] = jnp.where(own, f_ref[f, nt - 1], jnp.where(keep, got, 0.0))
    for f in range(8):
        for c in range(nt):
            at = t8_ref.at[f] if c == nt - 1 else f_ref.at[f, c]
            low_ref[f, c] = at[0:8]
            low_ref[8, c, f : f + 1] = at[8:9]
            high_ref[f, c] = at[ncols - 8 : ncols]
            high_ref[8, c, f : f + 1] = at[ncols - 9 : ncols - 8]
    s = sum_ref[0:1, :] + sum_in[0:1, :]
    chunk = [chunk_ref[k : k + 1, :] for k in range(4)]
    chunk[3] = chunk[3] + s
    block = jnp.concatenate(chunk, axis=0)
    for n in range(send_ref.shape[0]):
        send_ref[n] = block


def ghosts(got_ref, sel_ref, col_ref):
    n = got_ref.shape[0] // 4
    parts = []
    for r in range(4):
        m = got_ref[pl.ds(r, n, stride=4), :]
        h = m.astype(jnp.bfloat16)
        m = m - h.astype(F32)
        h2 = m.astype(jnp.bfloat16)
        h3 = (m - h2.astype(F32)).astype(jnp.bfloat16)
        parts.append(jnp.concatenate([h, h2, h3], axis=0))
    picked = jnp.dot(sel_ref[...], jnp.concatenate(parts, axis=1), preferred_element_type=F32)
    lane = lax.broadcasted_iota(jnp.int32, (sel_ref.shape[0], LANES), 1)
    col = col_ref[...] == (lane & 31)
    group = lane >> 5
    picked = [jnp.where(col, picked[:, r * LANES : (r + 1) * LANES], 0.0) for r in range(4)]
    out = []
    for f in range(5):
        vals = []
        for k in range(3):
            row, g = (k, f) if f < 4 else (3, k)
            vals.append(jnp.sum(jnp.where(group == g, picked[row], 0.0), axis=1, keepdims=True))
        out.append(vals)
    return out


def smooth_into(w_ref, g_ref, acc_ref, nf, start, tiles):
    nt = g_ref.shape[1]
    lane = lax.broadcasted_iota(jnp.int32, (8, LANES), 1)

    def one(f, i):
        row = start + i * 8
        mid, rolled = {}, {}
        for c in range(nt):
            x = [g_ref[f, c, pl.ds(row + a - 3, 8), :] for a in range(7)]
            for b in range(7):
                t = w_ref[0, b] * x[0]
                for a in range(1, 7):
                    t = t + w_ref[a, b] * x[a]
                if b == 3:
                    mid[c] = t
                else:
                    rolled[c, b] = pltpu.roll(t, (3 - b) % LANES, 1)
        for c in range(nt):
            t = mid[c]
            for b in range(3):
                t = t + (jnp.where(lane < 3 - b, rolled[(c - 1) % nt, b], rolled[c, b]) if nt > 1 else rolled[c, b])
            for b in range(4, 7):
                t = t + (jnp.where(lane >= LANES - (b - 3), rolled[(c + 1) % nt, b], rolled[c, b]) if nt > 1 else rolled[c, b])
            acc_ref[f, c, pl.ds(pl.multiple_of(i * 8, 8), 8), :] = t

    def body(step, _):
        one(step // tiles, step % tiles)
        return 0

    lax.fori_loop(0, nf * tiles, body, 0)


def lane_value(row, at):
    lane1 = lax.broadcasted_iota(jnp.int32, row.shape, 1)
    return jnp.sum(jnp.where(lane1 == at, row, 0.0), axis=1, keepdims=True)


def received_sums(got_ref):
    return jnp.sum(got_ref[pl.ds(3, got_ref.shape[0] // 4, stride=4), :], axis=0, keepdims=True)


def ghost_sums(w_ref, got_ref, sel_ref, col_ref, gg_ref, ga_ref, factor, edge, first, start, tiles):
    gh = ghosts(got_ref, sel_ref, col_ref)
    d, q = gh[0], gh[1]
    if first:
        oc = [jnp.where(v > 0.0, 1.0, 0.0) for v in q]
        rc = [1.0 / (0.6 * jnp.where(v > 0.0, v, 1.0)) for v in q]
        q = [oc[k] * overstress([gh[2 + m][k] for m in range(3)], rc[k])[1] for k in range(3)]
    vals = [[d[k] + factor * (1.0 - d[k]) * q[k] for k in range(3)]]
    for m in range(3):
        vals.append([gh[2 + m][k] * (1.0 - factor * q[k]) for k in range(3)])
    if first:
        vals.append(oc)
    shape = gg_ref.shape[2:]
    lane = lax.broadcasted_iota(jnp.int32, shape, 1)
    at = jnp.where(is_north(), edge, -4)
    for f, v in enumerate(vals):
        t = jnp.zeros(shape, F32)
        for k in range(3):
            t = jnp.where(lane == at + k, v[k], t)
        gg_ref[f, 0] = t
    smooth_into(w_ref, gg_ref, ga_ref, len(vals), start, tiles)


def coefficients(r, g, acc):
    x = [0.5 * g[0] + r * acc[0]] + [0.5 * g[2 + k] + r * acc[2 + k] for k in range(3)]
    y = [0.5 * g[1] + r * acc[1]] + [-(0.5 * g[5 + k] + r * acc[5 + k]) for k in range(3)]
    return x, y


def put_parts(g_ref, c, at, d, q, e):
    g_ref[0, c, at, :] = d
    g_ref[1, c, at, :] = (1.0 - d) * q
    for k in range(3):
        g_ref[2 + k, c, at, :] = e[k]
        g_ref[5 + k, c, at, :] = e[k] * q


def ahead_first(w_ref, f_ref, t8_ref, low_in, high_in, x_ref, y_ref, stat_ref, r_ref, edge_ref, g_ref, acc_ref):
    nt = f_ref.shape[1]
    ncols = f_ref.shape[2]
    n = x_ref.shape[2]

    def local(vals, c, row, nr):
        d, _, e, q, _, oc, rc = start_state(vals)
        at = slice(row, row + nr)
        put_parts(g_ref, c, at, d, q, e)
        g_ref[8, c, at, :] = oc
        if nr == 8:
            to = slice(row - 8, row)
            for k in range(3):
                stat_ref[k, c, to, :] = vals[k]
            stat_ref[3, c, to, :] = rc

    for c in range(nt):
        local([high_in[8, c, f : f + 1, :] for f in range(8)], c, PAD - 9, 1)
        local([high_in[f, c] for f in range(8)], c, PAD - 8, 8)
        for i in range(ncols // 8):
            at = slice(8 * i, 8 * i + 8)
            local([(t8_ref[f, at, :] if c == nt - 1 else f_ref[f, c, at, :]) for f in range(8)], c, PAD + 8 * i, 8)
        local([low_in[f, c] for f in range(8)], c, PAD + ncols, 8)
        local([low_in[8, c, f : f + 1, :] for f in range(8)], c, PAD + ncols + 8, 1)
    smooth_into(w_ref, g_ref, acc_ref, 9, 8, n // 8)
    for i in range(n // 8):
        at, to = slice(8 + 8 * i, 16 + 8 * i), slice(8 * i, 8 * i + 8)
        for c in range(nt - 1):
            r = 0.5 * g_ref[8, c, at, :] / (acc_ref[8, c, to, :] + 1.0)
            r_ref[c, to, :] = r
            x, y = coefficients(r, [g_ref[f, c, at, :] for f in range(8)], [acc_ref[f, c, to, :] for f in range(8)])
            for f in range(4):
                x_ref[f, c, to, :] = x[f]
                y_ref[f, c, to, :] = y[f]
        for f in range(9):
            edge_ref[f, to, :] = g_ref[f, nt - 1, at, :]
            edge_ref[9 + f, to, :] = acc_ref[f, nt - 1, to, :]


def ahead_later(skip, w_ref, dyn_in, r_ref, r8_ref, x_ref, y_ref, g_ref, acc_ref):
    nt = dyn_in.shape[1]
    n = x_ref.shape[2]
    for i in range(dyn_in.shape[2] // 8):
        at = slice(8 * i, 8 * i + 8)
        for c in range(nt):
            put_parts(g_ref, c, at, *[dyn_in[f, c, at, :] for f in range(2)], [dyn_in[2 + k, c, at, :] for k in range(3)])
    smooth_into(w_ref, g_ref, acc_ref, 8, 4, n // 8)
    for i in range(n // 8):
        at, to, fr = slice(4 + 8 * i, 12 + 8 * i), slice(8 * i, 8 * i + 8), slice(skip + 8 * i, skip + 8 * i + 8)
        for c in range(nt):
            r = r8_ref[fr, :] if c == nt - 1 else r_ref[c, fr, :]
            x, y = coefficients(r, [g_ref[f, c, at, :] for f in range(8)], [acc_ref[f, c, to, :] for f in range(8)])
            for f in range(4):
                x_ref[f, c, to, :] = x[f]
                y_ref[f, c, to, :] = y[f]


def next_state(c, at, to, new, stat_ref, dyn_ref):
    e, q, over = physics(new[0], new[1:], [stat_ref[k, c, at, :] for k in range(3)], stat_ref[3, c, at, :])
    dyn_ref[0, c, to, :] = new[0]
    dyn_ref[1, c, to, :] = q
    for k in range(3):
        dyn_ref[2 + k, c, to, :] = e[k]
    return over


def send_next(dyn_ref, own, excess, edge, chunk_ref, sum_ref):
    nt = dyn_ref.shape[1]
    tile = [dyn_ref[f, nt - 1, own, :] for f in range(5)]
    rows = tops(tile[:4], tile[4], edge - 1)
    s = total(excess)
    lane1 = lax.broadcasted_iota(jnp.int32, (1, LANES), 1)
    sums = jnp.where(lane1 == 96, s, 0.0)
    rows[3] = rows[3] + sums
    for k, row in enumerate(rows):
        chunk_ref[k : k + 1, :] = row
    zero = jnp.zeros((1, LANES), F32)
    for k in range(4):
        sum_ref[k : k + 1, :] = sums if k == 3 else zero


def after_first(
    nrows, ncols, w_ref, x_ref, y_ref, stat_ref, edge_ref, got_ref, sel_ref, col_ref,
    dyn_ref, r8_ref, chunk_ref, sum_ref, mean_ref, gg_ref, ga_ref,
):
    nt = x_ref.shape[1] + 1
    n = x_ref.shape[2]
    edge = nrows - (nt - 1) * LANES
    sums = received_sums(got_ref)
    count = lane_value(sums, 97) + 1.0
    mean = lane_value(sums, 96) / count
    factor = 1.0 / (1.0 + 2.0 * mean)
    lane1 = lax.broadcasted_iota(jnp.int32, mean_ref.shape, 1)
    mean_ref[...] = jnp.where(lane1 == 1, mean, count)
    lane = lax.broadcasted_iota(jnp.int32, (8, LANES), 1)
    f8 = jnp.broadcast_to(factor, (8, LANES))
    ghost_sums(w_ref, got_ref, sel_ref, col_ref, gg_ref, ga_ref, factor, edge, True, 8, n // 8)
    excess = jnp.zeros((8, LANES), F32)
    for i in range(n // 8):
        at = slice(8 * i, 8 * i + 8)
        own = PAD - 8 <= 8 * i < PAD - 8 + ncols
        for c in range(nt):
            if c == nt - 1:
                r = 0.5 * edge_ref[8, at, :] / (edge_ref[17, at, :] + ga_ref[4, 0, at, :] + 1.0)
                r8_ref[at, :] = r
                x, y = coefficients(r, [edge_ref[f, at, :] for f in range(8)], [edge_ref[9 + f, at, :] for f in range(8)])
                new = [x[f] + f8 * y[f] + r * ga_ref[f, 0, at, :] for f in range(4)]
            else:
                new = [x_ref[f, c, at, :] + f8 * y_ref[f, c, at, :] for f in range(4)]
            over = next_state(c, at, at, new, stat_ref, dyn_ref)
            if own:
                excess = excess + (jnp.where(lane < edge, over, 0.0) if c == nt - 1 else over)
    send_next(dyn_ref, slice(PAD - 8, PAD - 8 + ncols), excess, edge, chunk_ref, sum_ref)


def after_second(
    nrows, ncols, w_ref, x_ref, y_ref, stat_ref, r8_ref, got_ref, sel_ref, col_ref, mean_in,
    dyn_ref, chunk_ref, sum_ref, mean_ref, gg_ref, ga_ref,
):
    nt = x_ref.shape[1]
    n = x_ref.shape[2]
    edge = nrows - (nt - 1) * LANES
    mean = lane_value(received_sums(got_ref), 96) / lane_value(mean_in[0:1, :], 0)
    factor = 1.0 / (1.0 + 2.0 * mean)
    lane1 = lax.broadcasted_iota(jnp.int32, mean_ref.shape, 1)
    mean_ref[...] = jnp.where(lane1 == 2, mean, mean_in[...])
    lane = lax.broadcasted_iota(jnp.int32, (8, LANES), 1)
    row = lax.broadcasted_iota(jnp.int32, (8, LANES), 0)
    f8 = jnp.broadcast_to(factor, (8, LANES))
    ghost_sums(w_ref, got_ref, sel_ref, col_ref, gg_ref, ga_ref, factor, edge, False, 12, n // 8)
    excess = jnp.zeros((8, LANES), F32)
    for i in range(n // 8):
        at, to = slice(4 + 8 * i, 12 + 8 * i), slice(8 * i, 8 * i + 8)
        for c in range(nt):
            new = [x_ref[f, c, to, :] + f8 * y_ref[f, c, to, :] for f in range(4)]
            if c == nt - 1:
                new = [new[f] + r8_ref[at, :] * ga_ref[f, 0, to, :] for f in range(4)]
            over = next_state(c, at, to, new, stat_ref, dyn_ref)
            if 8 * i < 4:
                over = jnp.where(row >= 4, over, 0.0)
            if 8 * i + 8 > 4 + ncols:
                over = jnp.where(row < 4, over, 0.0)
            excess = excess + (jnp.where(lane < edge, over, 0.0) if c == nt - 1 else over)
    send_next(dyn_ref, slice(4, 4 + ncols), excess, edge, chunk_ref, sum_ref)


def after_third(
    nrows, ncols, w_ref, x_ref, y_ref, r8_ref, got_ref, sel_ref, col_ref, mean_in,
    stress_ref, damage_ref, mean_ref, gg_ref, ga_ref,
):
    nt = x_ref.shape[1]
    edge = nrows - (nt - 1) * LANES
    row = mean_in[0:1, :]
    mean = lane_value(received_sums(got_ref), 96) / lane_value(row, 0)
    factor = 1.0 / (1.0 + 2.0 * mean)
    for at, one in enumerate((lane_value(row, 1), lane_value(row, 2), mean)):
        mean_ref[at] = jnp.sum(one)
    f8 = jnp.broadcast_to(factor, (8, LANES))
    ghost_sums(w_ref, got_ref, sel_ref, col_ref, gg_ref, ga_ref, factor, edge, False, PAD, ncols // 8)
    for c in range(nt):
        w = min(LANES, nrows - c * LANES)
        for i in range(ncols // 8):
            at = slice(8 * i, 8 * i + 8)
            for f in range(4):
                v = x_ref[f, c, at, :] + f8 * y_ref[f, c, at, :]
                if c == nt - 1:
                    v = v + r8_ref[8 + 8 * i : 16 + 8 * i, :] * ga_ref[f, 0, at, :]
                if f == 0:
                    damage_ref[at, c * LANES : c * LANES + w] = v[:, 0:w]
                else:
                    stress_ref[f - 1, at, c * LANES : c * LANES + w] = v[:, 0:w]


def step(strain_rate, stress_start, concentration, cell_class, land_mask, fold_partner, kernel_weights):
    ncols, nrows = concentration.shape
    nt = -(-nrows // LANES)
    nlon = lax.axis_size("lon")
    nlat = lax.axis_size("lat")
    rows = ncols + 2 * PAD
    n1, n2 = rows - 16, rows - 24
    sds = lambda *s: jax.ShapeDtypeStruct(s, F32)
    vmem = lambda *s: pltpu.VMEM(s, F32)

    def call(body, flops, *args, weights=True, **kw):
        given = args if not weights else (kernel_weights, *args)
        return pl.pallas_call(
            body, in_specs=([SM] if weights else []) + [VM] * len(args), cost_estimate=cost(flops, flops),
            compiler_params=small(), **kw,
        )(*given)

    columns = (lax.axis_index("lon") * ncols - PAD + jnp.arange(rows, dtype=jnp.int32)) % (ncols * nlon)
    partner = jnp.take(fold_partner, columns)
    sel = (partner[:, None] // ncols == jnp.arange(nlon)[None, :]).astype(jnp.bfloat16)
    sel = jnp.concatenate([sel, sel, sel], axis=1)
    col = jnp.broadcast_to((partner % ncols)[:, None], (rows, LANES)).astype(jnp.int32)

    given = (strain_rate, stress_start, concentration, cell_class, land_mask)
    f, lat_out, chunk, sums = pl.pallas_call(
        functools.partial(first_kernel, nrows),
        out_shape=(sds(8, nt, ncols, LANES), sds(8, ncols, LANES), sds(4, LANES), sds(8, LANES)),
        in_specs=[pl.BlockSpec(memory_space=pltpu.HBM)] * 5, out_specs=(VM,) * 4,
        scratch_shapes=[pltpu.VMEM(a.shape, a.dtype) for a in given] + [pltpu.SemaphoreType.DMA((5,))],
        cost_estimate=cost(4000000, 2000000), compiler_params=small(), name="first",
    )(*(pltpu.with_memory_space_constraint(a, pltpu.HBM) for a in given))
    swap = [(i, nlat - 1 - i) for i in range(nlat)]
    lat_in = lax.ppermute(lat_out, "lat", swap)
    sum_in = lax.ppermute(sums, "lat", swap)
    t8, low, high, send = call(
        functools.partial(second_kernel, nrows), 400000, f, lat_in, chunk, sums, sum_in, weights=False,
        out_shape=(sds(8, ncols, LANES), sds(9, nt, 8, LANES), sds(9, nt, 8, LANES), sds(nlon, 4, LANES)), out_specs=(VM,) * 4,
    )
    up = [(i, (i + 1) % nlon) for i in range(nlon)]
    down = [(j, i) for i, j in up]
    high_in = lax.ppermute(high, "lon", up)
    low_in = lax.ppermute(low, "lon", down)
    got = lax.all_to_all(send, "lon", 0, 0, tiled=True).reshape(nlon * 4, LANES)

    x, y, stat, r, edge = call(
        ahead_first, 60000000, f, t8, low_in, high_in,
        out_shape=(sds(4, nt - 1, n1, LANES), sds(4, nt - 1, n1, LANES), sds(4, nt, n1, LANES), sds(nt - 1, n1, LANES), sds(18, n1, LANES)),
        out_specs=(VM,) * 5, scratch_shapes=[vmem(9, nt, rows, LANES), vmem(9, nt, n1, LANES)],
    )
    dyn, r8, chunk, sums, mean = call(
        functools.partial(after_first, nrows, ncols), 4000000, x, y, stat, edge, got, sel, col,
        out_shape=(sds(5, nt, n1, LANES), sds(n1, LANES), sds(4, LANES), sds(4, LANES), sds(8, LANES)),
        out_specs=(VM,) * 5, scratch_shapes=[vmem(5, 1, rows, LANES), vmem(5, 1, n1, LANES)],
    )

    def spread(chunk, sums):
        chunk = chunk + lax.ppermute(sums, "lat", swap)
        send = jnp.broadcast_to(chunk[None], (nlon, 4, LANES))
        return lax.all_to_all(send, "lon", 0, 0, tiled=True).reshape(nlon * 4, LANES)

    got = spread(chunk, sums)
    x, y = call(
        functools.partial(ahead_later, 4), 50000000, dyn, r, r8,
        out_shape=(sds(4, nt, n2, LANES), sds(4, nt, n2, LANES)), out_specs=(VM,) * 2,
        scratch_shapes=[vmem(8, nt, n1, LANES), vmem(8, nt, n2, LANES)],
    )
    dyn, chunk, sums, mean = call(
        functools.partial(after_second, nrows, ncols), 4000000, x, y, stat, r8, got, sel, col, mean,
        out_shape=(sds(5, nt, n2, LANES), sds(4, LANES), sds(4, LANES), sds(8, LANES)),
        out_specs=(VM,) * 4, scratch_shapes=[vmem(4, 1, rows, LANES), vmem(4, 1, n2, LANES)],
    )
    got = spread(chunk, sums)
    x, y = call(
        functools.partial(ahead_later, 8), 40000000, dyn, r, r8,
        out_shape=(sds(4, nt, ncols, LANES), sds(4, nt, ncols, LANES)), out_specs=(VM,) * 2,
        scratch_shapes=[vmem(8, nt, n2, LANES), vmem(8, nt, ncols, LANES)],
    )
    return call(
        functools.partial(after_third, nrows, ncols), 4000000, x, y, r8, got, sel, col, mean,
        out_shape=(sds(3, ncols, nrows), sds(ncols, nrows), sds(ITERS)), out_specs=(VM, VM, SM),
        scratch_shapes=[vmem(4, 1, rows, LANES), vmem(4, 1, ncols, LANES)],
    )


def solution(mesh):
    in_specs = (
        P(None, "lon", "lat"),
        P(None, "lon", "lat"),
        P("lon", "lat"),
        P(("member", "lon"), "lat"),
        P("lon", "lat"),
        P(),
        P(),
    )
    out_specs = (P(None, ("member", "lon"), "lat"), P(("member", "lon"), "lat"), P("member"))
    return jax.shard_map(step, mesh=mesh, in_specs=in_specs, out_specs=out_specs, check_vma=False)
```

```python
import functools
import jax
import jax.numpy as jnp
from jax import lax
from jax.experimental import pallas as pl
from jax.experimental.pallas import tpu as pltpu
from jax.sharding import PartitionSpec as P


ITERS = 3
HALO = 9
LANES = 128
PAD = 16
F32 = jnp.float32
VM = pl.BlockSpec(memory_space=pltpu.VMEM)
SM = pl.BlockSpec(memory_space=pltpu.SMEM)


def small():
    return pltpu.CompilerParams(vmem_limit_bytes=12 * 1024 * 1024)


def is_north():
    return lax.axis_index("lat") == lax.axis_size("lat") - 1


def cost(flops, size):
    return pl.CostEstimate(flops=flops, bytes_accessed=size, transcendentals=0)


def overstress(e, rc):
    half = (e[0] - e[1]) * 0.5
    tau = jnp.sqrt(half * half + e[2] * e[2] + 0.25)
    over = jnp.maximum((tau + 0.35 * (e[0] + e[1])) * rc, 1.0)
    return over - 1.0, 1.0 - 1.0 / over


def physics(damage, stress, bl, rc):
    keep = 1.0 - damage
    k2 = keep * keep
    g = k2 / (k2 + 0.5)
    e = [g * (stress[k] + keep * bl[k]) for k in range(3)]
    excess, q = overstress(e, rc)
    return e, q, excess


def tops(tiles, single, at):
    t = jnp.concatenate(tiles, axis=0).T
    rows = [t[at - k : at - k + 1, :] for k in range(3)]
    parts = [single] + [pltpu.roll(single, k, 1) for k in (1, 2)] + [jnp.zeros_like(single)]
    return rows + [jnp.concatenate(parts, axis=0).T[at : at + 1, :]]


def total(x):
    return jnp.sum(jnp.sum(x, axis=0, keepdims=True), axis=1, keepdims=True)


def first_kernel(nrows, *refs):
    given, (f_ref, lat_out, chunk_ref, sum_ref), held, sem = refs[:5], refs[5:9], refs[9:14], refs[14]
    copies = [pltpu.make_async_copy(a, b, sem.at[n]) for n, (a, b) in enumerate(zip(given, held, strict=True))]
    for n in (2, 4, 3, 0, 1):
        copies[n].start()
    strain, stress, conc, cls, mask = held
    nt = f_ref.shape[1]
    ncols = conc.shape[0]
    f_ref[:, nt - 1] = jnp.zeros((8, ncols, LANES), F32)
    parts = [(c, min(LANES, nrows - c * LANES), slice(c * LANES, min(nrows, (c + 1) * LANES))) for c in range(nt)]
    for n in (2, 4, 3):
        copies[n].wait()
    for c, w, sl in parts:
        con = conc[:, sl]
        oc = mask[:, sl].astype(F32)
        f_ref[0, c, :, 0:w] = oc * con * jnp.exp(-2.0 * (1.0 - con))
        f_ref[6, c, :, 0:w] = oc * con
        f_ref[7, c, :, 0:w] = oc * 0.1 * cls[:, sl].astype(F32) * con
    copies[0].wait()
    third = 1.0 / 3.0
    for c, w, sl in parts:
        e1, e2, e3 = (strain[k, :, sl] for k in range(3))
        base = f_ref[0, c, :, 0:w]
        f_ref[0, c, :, 0:w] = base * ((e1 + e2 * third) * 1.125)
        f_ref[1, c, :, 0:w] = base * ((e2 + e1 * third) * 1.125)
        f_ref[2, c, :, 0:w] = base * (e3 * (0.75 * 1.125))
    copies[1].wait()
    for c, w, sl in parts:
        oc = jnp.where(f_ref[6, c, :, 0:w] > 0.0, 1.0, 0.0)
        for k in range(3):
            f_ref[3 + k, c, :, 0:w] = oc * stress[k, :, sl]
    excess = jnp.zeros((ncols, LANES), F32)
    count = jnp.zeros((ncols, LANES), F32)
    for c in range(nt):
        d, mc, e, _, over, oc, _ = start_state([f_ref[k, c] for k in range(8)])
        excess = excess + over
        count = count + oc
    at = nrows - 1 - (nt - 1) * LANES
    rows = tops([d, mc, e[0], e[1]], e[2], at)
    s = total(excess)
    n = total(count)
    lane1 = lax.broadcasted_iota(jnp.int32, (1, LANES), 1)
    sums = jnp.where(lane1 == 96, s, 0.0) + jnp.where(lane1 == 97, n, 0.0)
    for k, row in enumerate(rows):
        chunk_ref[k : k + 1, :] = row
    sum_ref[...] = jnp.broadcast_to(sums, sum_ref.shape)
    north = is_north()
    for f in range(8):
        lat_out[f] = jnp.where(north, f_ref[f, 0], f_ref[f, nt - 1])


def start_state(vals):
    bl, st, mc, d = vals[0:3], vals[3:6], vals[6], vals[7]
    oc = jnp.where(mc > 0.0, 1.0, 0.0)
    rc = oc / (0.6 * jnp.where(mc > 0.0, mc, 1.0))
    e, q, over = physics(d, st, bl, rc)
    return d, mc, e, q, over, oc, rc


def second_kernel(nrows, f_in, lat_in, chunk_ref, sum_ref, sum_in, f_ref, low_ref, high_ref, send_ref):
    nt = f_ref.shape[1]
    ncols = f_ref.shape[2]
    edge = nrows - (nt - 1) * LANES
    lane = lax.broadcasted_iota(jnp.int32, (ncols, LANES), 1)
    north = is_north()
    own = lane < edge
    keep = jnp.where(north, (lane >= LANES - HALO).astype(jnp.int32), ((lane >= edge) & (lane < edge + HALO)).astype(jnp.int32)) > 0
    for f in range(8):
        got = jnp.where(north, pltpu.roll(lat_in[f], (LANES - edge) % LANES, 1), pltpu.roll(lat_in[f], edge, 1))
        f_ref[f, nt - 1] = jnp.where(own, f_ref[f, nt - 1], jnp.where(keep, got, 0.0))
    for f in range(8):
        for c in range(nt):
            low_ref[f, c] = f_ref[f, c, 0:8]
            low_ref[8, c, f : f + 1] = f_ref[f, c, 8:9]
            high_ref[f, c] = f_ref[f, c, ncols - 8 : ncols]
            high_ref[8, c, f : f + 1] = f_ref[f, c, ncols - 9 : ncols - 8]
    s = sum_ref[0:1, :] + sum_in[0:1, :]
    chunk = [chunk_ref[k : k + 1, :] for k in range(4)]
    chunk[3] = chunk[3] + s
    block = jnp.concatenate(chunk, axis=0)
    for n in range(send_ref.shape[0]):
        send_ref[n] = block


def ghosts(got_ref, partner_ref):
    n = got_ref.shape[0] // 4
    parts = []
    for r in range(4):
        m = got_ref[pl.ds(r, n, stride=4), :]
        h = m.astype(jnp.bfloat16)
        m = m - h.astype(F32)
        h2 = m.astype(jnp.bfloat16)
        h3 = (m - h2.astype(F32)).astype(jnp.bfloat16)
        parts.append(jnp.concatenate([h, h2, h3], axis=0))
    partner = partner_ref[...]
    rows = partner.shape[0]
    source, place = partner >> 5, partner & 31
    one_hot = source[:, 0 : 3 * n] == (lax.broadcasted_iota(jnp.int32, (rows, 3 * n), 1) % n)
    sel = jnp.where(one_hot, 1.0, 0.0).astype(jnp.bfloat16)
    picked = jnp.dot(sel, jnp.concatenate(parts, axis=1), preferred_element_type=F32)
    lane = lax.broadcasted_iota(jnp.int32, (rows, LANES), 1)
    col = place == (lane & 31)
    group = lane >> 5
    picked = [jnp.where(col, picked[:, r * LANES : (r + 1) * LANES], 0.0) for r in range(4)]
    out = []
    for f in range(5):
        vals = []
        for k in range(3):
            row, g = (k, f) if f < 4 else (3, k)
            vals.append(jnp.sum(jnp.where(group == g, picked[row], 0.0), axis=1, keepdims=True))
        out.append(vals)
    return out


def smooth_into(w_ref, g_ref, acc_ref, nf, start, tiles):
    nt = g_ref.shape[1]
    lane = lax.broadcasted_iota(jnp.int32, (8, LANES), 1)

    def one(f, i):
        row = start + i * 8
        mid, rolled = {}, {}
        for c in range(nt):
            x = [g_ref[f, c, pl.ds(row + a - 3, 8), :] for a in range(7)]
            for b in range(7):
                t = w_ref[0, b] * x[0]
                for a in range(1, 7):
                    t = t + w_ref[a, b] * x[a]
                if b == 3:
                    mid[c] = t
                else:
                    rolled[c, b] = pltpu.roll(t, (3 - b) % LANES, 1)
        for c in range(nt):
            t = mid[c]
            for b in range(3):
                t = t + (jnp.where(lane < 3 - b, rolled[(c - 1) % nt, b], rolled[c, b]) if nt > 1 else rolled[c, b])
            for b in range(4, 7):
                t = t + (jnp.where(lane >= LANES - (b - 3), rolled[(c + 1) % nt, b], rolled[c, b]) if nt > 1 else rolled[c, b])
            acc_ref[f, c, pl.ds(pl.multiple_of(i * 8, 8), 8), :] = t

    def body(step, _):
        one(step // tiles, step % tiles)
        return 0

    lax.fori_loop(0, nf * tiles, body, 0)


def lane_value(row, at):
    lane1 = lax.broadcasted_iota(jnp.int32, row.shape, 1)
    return jnp.sum(jnp.where(lane1 == at, row, 0.0), axis=1, keepdims=True)


def received_sums(got_ref):
    return jnp.sum(got_ref[pl.ds(3, got_ref.shape[0] // 4, stride=4), :], axis=0, keepdims=True)


def edge_weights(w_ref, wl_ref, edge):
    lane = lax.broadcasted_iota(jnp.int32, (1, LANES), 1)
    at = jnp.where(is_north(), edge - 1, -4)
    for k in range(3):
        for a in range(7):
            t = jnp.zeros((1, LANES), F32)
            for m in range(3 - k):
                t = jnp.where(lane == at - m, w_ref[a, 4 + k + m], t)
            wl_ref[7 * k + a : 7 * k + a + 1, :] = t


def ghost_sums(wl_ref, got_ref, partner_ref, gg_ref, factor, first, start, tiles):
    gh = ghosts(got_ref, partner_ref)
    d, q = gh[0], gh[1]
    if first:
        oc = [jnp.where(v > 0.0, 1.0, 0.0) for v in q]
        rc = [1.0 / (0.6 * jnp.where(v > 0.0, v, 1.0)) for v in q]
        q = [oc[k] * overstress([gh[2 + m][k] for m in range(3)], rc[k])[1] for k in range(3)]
    vals = [[d[k] + factor * (1.0 - d[k]) * q[k] for k in range(3)]]
    for m in range(3):
        vals.append([gh[2 + m][k] * (1.0 - factor * q[k]) for k in range(3)])
    if first:
        vals.append(oc)
    for f, v in enumerate(vals):
        for k in range(3):
            gg_ref[3 * f + k] = jnp.broadcast_to(v[k], gg_ref.shape[1:])
    wl = [wl_ref[n : n + 1, :] for n in range(21)]
    out = []
    for f in range(len(vals)):
        sums = []
        for i in range(tiles):
            row = start + 8 * i
            t = None
            for k in range(3):
                u = gg_ref[3 * f + k, row - 3 : row + 5, :] * wl[7 * k]
                for a in range(1, 7):
                    u = u + gg_ref[3 * f + k, row + a - 3 : row + a + 5, :] * wl[7 * k + a]
                t = u if t is None else t + u
            sums.append(t)
        out.append(sums)
    return out


def coefficients(r, g, acc):
    x = [0.5 * g[0] + r * acc[0]] + [0.5 * g[2 + k] + r * acc[2 + k] for k in range(3)]
    y = [0.5 * g[1] + r * acc[1]] + [-(0.5 * g[5 + k] + r * acc[5 + k]) for k in range(3)]
    return x, y


def put_parts(g_ref, c, at, d, q, e):
    g_ref[0, c, at, :] = d
    g_ref[1, c, at, :] = (1.0 - d) * q
    for k in range(3):
        g_ref[2 + k, c, at, :] = e[k]
        g_ref[5 + k, c, at, :] = e[k] * q


def ahead_first(
    edge, w_ref, f_ref, low_hbm, high_hbm, y_hbm, stat_ref, r_ref, edge_ref, wl_ref,
    g_ref, acc_ref, low_in, high_in, y_ref, sem, y_sem,
):
    copies = [pltpu.make_async_copy(high_hbm, high_in, sem.at[0]), pltpu.make_async_copy(low_hbm, low_in, sem.at[1])]
    for copy in copies:
        copy.start()
    nt = f_ref.shape[1]
    ncols = f_ref.shape[2]
    n = stat_ref.shape[2]
    edge_weights(w_ref, wl_ref, edge)

    def local(vals, c, row, nr):
        d, _, e, q, _, oc, rc = start_state(vals)
        at = slice(row, row + nr)
        put_parts(g_ref, c, at, d, q, e)
        g_ref[8, c, at, :] = oc
        if nr == 8:
            to = slice(row - 8, row)
            for k in range(3):
                stat_ref[k, c, to, :] = vals[k]
            stat_ref[3, c, to, :] = rc

    for c in range(nt):
        for i in range(ncols // 8):
            local([f_ref[f, c, 8 * i : 8 * i + 8, :] for f in range(8)], c, PAD + 8 * i, 8)
    for copy in copies:
        copy.wait()
    for c in range(nt):
        local([high_in[8, c, f : f + 1, :] for f in range(8)], c, PAD - 9, 1)
        local([high_in[f, c] for f in range(8)], c, PAD - 8, 8)
        local([low_in[f, c] for f in range(8)], c, PAD + ncols, 8)
        local([low_in[8, c, f : f + 1, :] for f in range(8)], c, PAD + ncols + 8, 1)
    smooth_into(w_ref, g_ref, acc_ref, 9, 8, n // 8)
    for i in range(n // 8):
        at, to = slice(8 + 8 * i, 16 + 8 * i), slice(8 * i, 8 * i + 8)
        for c in range(nt - 1):
            r = 0.5 * g_ref[8, c, at, :] / (acc_ref[8, c, to, :] + 1.0)
            r_ref[c, to, :] = r
            x, y = coefficients(r, [g_ref[f, c, at, :] for f in range(8)], [acc_ref[f, c, to, :] for f in range(8)])
            for f in range(4):
                y_ref[i, f, c] = x[f]
                y_ref[i, 4 + f, c] = y[f]
        pltpu.make_async_copy(y_ref.at[i], y_hbm.at[i], y_sem.at[i]).start()
        for f in range(9):
            edge_ref[f, to, :] = g_ref[f, nt - 1, at, :]
            edge_ref[9 + f, to, :] = acc_ref[f, nt - 1, to, :]
    for i in range(n // 8):
        pltpu.make_async_copy(y_ref.at[i], y_hbm.at[i], y_sem.at[i]).wait()


def ahead_later(skip, w_ref, dyn_in, r_ref, r8_ref, y_hbm, g_ref, acc_ref, y_ref, y_sem):
    nt = dyn_in.shape[1]
    n = 8 * y_ref.shape[0]
    for i in range(dyn_in.shape[2] // 8):
        at = slice(8 * i, 8 * i + 8)
        for c in range(nt):
            put_parts(g_ref, c, at, *[dyn_in[f, c, at, :] for f in range(2)], [dyn_in[2 + k, c, at, :] for k in range(3)])
    smooth_into(w_ref, g_ref, acc_ref, 8, 4, n // 8)
    for i in range(n // 8):
        at, to, fr = slice(4 + 8 * i, 12 + 8 * i), slice(8 * i, 8 * i + 8), slice(skip + 8 * i, skip + 8 * i + 8)
        for c in range(nt):
            r = r8_ref[fr, :] if c == nt - 1 else r_ref[c, fr, :]
            x, y = coefficients(r, [g_ref[f, c, at, :] for f in range(8)], [acc_ref[f, c, to, :] for f in range(8)])
            for f in range(4):
                y_ref[i, f, c] = x[f]
                y_ref[i, 4 + f, c] = y[f]
        pltpu.make_async_copy(y_ref.at[i], y_hbm.at[i], y_sem.at[i]).start()
    for i in range(n // 8):
        pltpu.make_async_copy(y_ref.at[i], y_hbm.at[i], y_sem.at[i]).wait()


def next_state(c, at, to, new, stat_ref, dyn_ref):
    e, q, over = physics(new[0], new[1:], [stat_ref[k, c, at, :] for k in range(3)], stat_ref[3, c, at, :])
    dyn_ref[0, c, to, :] = new[0]
    dyn_ref[1, c, to, :] = q
    for k in range(3):
        dyn_ref[2 + k, c, to, :] = e[k]
    return over


def send_next(dyn_ref, own, excess, edge, chunk_ref, sum_ref):
    nt = dyn_ref.shape[1]
    tile = [dyn_ref[f, nt - 1, own, :] for f in range(5)]
    rows = tops(tile[:4], tile[4], edge - 1)
    s = total(excess)
    lane1 = lax.broadcasted_iota(jnp.int32, (1, LANES), 1)
    sums = jnp.where(lane1 == 96, s, 0.0)
    rows[3] = rows[3] + sums
    for k, row in enumerate(rows):
        chunk_ref[k : k + 1, :] = row
    zero = jnp.zeros((1, LANES), F32)
    for k in range(4):
        sum_ref[k : k + 1, :] = sums if k == 3 else zero


def after_first(
    edge, ncols, wl_ref, y_hbm, stat_ref, edge_ref, got_ref, partner_ref,
    dyn_ref, r8_ref, chunk_ref, sum_ref, mean_ref, gg_ref, y_ref, sem,
):
    copies = [pltpu.make_async_copy(y_hbm.at[i], y_ref.at[i], sem.at[i]) for i in range(y_ref.shape[0])]
    for copy in copies:
        copy.start()
    nt = y_ref.shape[2] + 1
    n = 8 * y_ref.shape[0]
    sums = received_sums(got_ref)
    count = lane_value(sums, 97) + 1.0
    mean = lane_value(sums, 96) / count
    factor = 1.0 / (1.0 + 2.0 * mean)
    lane1 = lax.broadcasted_iota(jnp.int32, mean_ref.shape, 1)
    mean_ref[...] = jnp.where(lane1 == 1, mean, count)
    lane = lax.broadcasted_iota(jnp.int32, (8, LANES), 1)
    f8 = jnp.broadcast_to(factor, (8, LANES))
    ga = ghost_sums(wl_ref, got_ref, partner_ref, gg_ref, factor, True, 8, n // 8)
    excess = jnp.zeros((8, LANES), F32)
    for i in range(n // 8):
        copies[i].wait()
        at = slice(8 * i, 8 * i + 8)
        own = PAD - 8 <= 8 * i < PAD - 8 + ncols
        for c in range(nt):
            if c == nt - 1:
                r = 0.5 * edge_ref[8, at, :] / (edge_ref[17, at, :] + ga[4][i] + 1.0)
                r8_ref[at, :] = r
                x, y = coefficients(r, [edge_ref[f, at, :] for f in range(8)], [edge_ref[9 + f, at, :] for f in range(8)])
                new = [x[f] + f8 * y[f] + r * ga[f][i] for f in range(4)]
            else:
                new = [y_ref[i, f, c] + f8 * y_ref[i, 4 + f, c] for f in range(4)]
            over = next_state(c, at, at, new, stat_ref, dyn_ref)
            if own:
                excess = excess + (jnp.where(lane < edge, over, 0.0) if c == nt - 1 else over)
    send_next(dyn_ref, slice(PAD - 8, PAD - 8 + ncols), excess, edge, chunk_ref, sum_ref)


def after_second(
    edge, ncols, wl_ref, y_hbm, stat_ref, r8_ref, got_ref, partner_ref, mean_in,
    dyn_ref, chunk_ref, sum_ref, mean_ref, gg_ref, y_ref, sem,
):
    copies = [pltpu.make_async_copy(y_hbm.at[i], y_ref.at[i], sem.at[i]) for i in range(y_ref.shape[0])]
    for copy in copies:
        copy.start()
    nt = y_ref.shape[2]
    n = 8 * y_ref.shape[0]
    mean = lane_value(received_sums(got_ref), 96) / lane_value(mean_in[0:1, :], 0)
    factor = 1.0 / (1.0 + 2.0 * mean)
    lane1 = lax.broadcasted_iota(jnp.int32, mean_ref.shape, 1)
    mean_ref[...] = jnp.where(lane1 == 2, mean, mean_in[...])
    lane = lax.broadcasted_iota(jnp.int32, (8, LANES), 1)
    row = lax.broadcasted_iota(jnp.int32, (8, LANES), 0)
    f8 = jnp.broadcast_to(factor, (8, LANES))
    ga = ghost_sums(wl_ref, got_ref, partner_ref, gg_ref, factor, False, 12, n // 8)
    excess = jnp.zeros((8, LANES), F32)
    for i in range(n // 8):
        copies[i].wait()
        at, to = slice(4 + 8 * i, 12 + 8 * i), slice(8 * i, 8 * i + 8)
        for c in range(nt):
            new = [y_ref[i, f, c] + f8 * y_ref[i, 4 + f, c] for f in range(4)]
            if c == nt - 1:
                new = [new[f] + r8_ref[at, :] * ga[f][i] for f in range(4)]
            over = next_state(c, at, to, new, stat_ref, dyn_ref)
            if 8 * i < 4:
                over = jnp.where(row >= 4, over, 0.0)
            if 8 * i + 8 > 4 + ncols:
                over = jnp.where(row < 4, over, 0.0)
            excess = excess + (jnp.where(lane < edge, over, 0.0) if c == nt - 1 else over)
    send_next(dyn_ref, slice(4, 4 + ncols), excess, edge, chunk_ref, sum_ref)


def after_third(
    nrows, wl_ref, y_hbm, r8_ref, got_ref, partner_ref, mean_in,
    stress_hbm, damage_hbm, mean_ref, gg_ref, y_ref, out_ref, sem, out_sem,
):
    copies = [pltpu.make_async_copy(y_hbm.at[i], y_ref.at[i], sem.at[i]) for i in range(y_ref.shape[0])]
    for copy in copies:
        copy.start()
    nt = y_ref.shape[2]
    ncols = 8 * y_ref.shape[0]
    row = mean_in[0:1, :]
    mean = lane_value(received_sums(got_ref), 96) / lane_value(row, 0)
    factor = 1.0 / (1.0 + 2.0 * mean)
    for at, one in enumerate((lane_value(row, 1), lane_value(row, 2), mean)):
        mean_ref[at] = jnp.sum(one)
    f8 = jnp.broadcast_to(factor, (8, LANES))
    ga = ghost_sums(wl_ref, got_ref, partner_ref, gg_ref, factor, False, PAD, ncols // 8)
    outs = []
    for i in range(ncols // 8):
        copies[i].wait()
        at = slice(8 * i, 8 * i + 8)
        for f in range(4):
            for c in range(nt):
                w = min(LANES, nrows - c * LANES)
                v = y_ref[i, f, c] + f8 * y_ref[i, 4 + f, c]
                if c == nt - 1:
                    v = v + r8_ref[8 + 8 * i : 16 + 8 * i, :] * ga[f][i]
                out_ref[f, at, c * LANES : c * LANES + w] = v[:, 0:w]
            to = damage_hbm.at[pl.ds(8 * i, 8)] if f == 0 else stress_hbm.at[f - 1, pl.ds(8 * i, 8)]
            outs.append(pltpu.make_async_copy(out_ref.at[f, pl.ds(8 * i, 8)], to, out_sem.at[4 * i + f]))
            outs[-1].start()
    for one in outs:
        one.wait()


def step(strain_rate, stress_start, concentration, cell_class, land_mask, fold_partner, kernel_weights):
    ncols, nrows = concentration.shape
    nt = -(-nrows // LANES)
    edge = nrows - (nt - 1) * LANES
    nlon = lax.axis_size("lon")
    nlat = lax.axis_size("lat")
    rows = ncols + 2 * PAD
    n1, n2 = rows - 16, rows - 24
    sds = lambda *s: jax.ShapeDtypeStruct(s, F32)
    vmem = lambda *s: pltpu.VMEM(s, F32)
    dma = lambda n: pltpu.SemaphoreType.DMA((n,))
    far = lambda a: pltpu.with_memory_space_constraint(a, pltpu.HBM)
    hbm = pl.BlockSpec(memory_space=pltpu.HBM)
    anywhere = pl.BlockSpec(memory_space=pl.ANY)
    hds = lambda *s: pltpu.HBM(s, F32)

    def call(body, flops, args, out_shape, scratch=(), weights=False, in_far=(), in_any=(), out_far=(), scalars=(), **kw):
        specs = [hbm if n in in_far else anywhere if n in in_any else VM for n in range(len(args))]
        args = [far(a) if n in in_far else a for n, a in enumerate(args)]
        return pl.pallas_call(
            body, in_specs=[SM] * weights + specs, out_shape=out_shape, scratch_shapes=scratch,
            out_specs=tuple(hbm if n in out_far else SM if n in scalars else VM for n in range(len(out_shape))),
            cost_estimate=cost(flops, flops), compiler_params=small(), **kw,
        )(*[kernel_weights] * weights, *args)

    columns = (lax.axis_index("lon") * ncols - PAD + jnp.arange(rows, dtype=jnp.int32)) % (ncols * nlon)
    partner = jnp.broadcast_to(jnp.take(fold_partner, columns)[:, None], (rows, LANES))

    given = (strain_rate, stress_start, concentration, cell_class, land_mask)
    f, lat_out, chunk, sums = call(
        functools.partial(first_kernel, nrows), 4000000, given,
        (sds(8, nt, ncols, LANES), sds(8, ncols, LANES), sds(4, LANES), sds(8, LANES)),
        [pltpu.VMEM(a.shape, a.dtype) for a in given] + [dma(5)], in_far=range(5),
    )
    swap = [(i, nlat - 1 - i) for i in range(nlat)]
    lat_in = lax.ppermute(lat_out, "lat", swap)
    sum_in = lax.ppermute(sums, "lat", swap)
    f, low, high, send = call(
        functools.partial(second_kernel, nrows), 400000, (f, lat_in, chunk, sums, sum_in),
        (sds(8, nt, ncols, LANES), sds(9, nt, 8, LANES), sds(9, nt, 8, LANES), sds(nlon, 4, LANES)), input_output_aliases={0: 0},
    )
    up = [(i, (i + 1) % nlon) for i in range(nlon)]
    down = [(j, i) for i, j in up]
    high_in = lax.ppermute(high, "lon", up)
    low_in = lax.ppermute(low, "lon", down)
    got = lax.all_to_all(send, "lon", 0, 0, tiled=True).reshape(nlon * 4, LANES)

    strip = vmem(9, nt, 8, LANES)
    y1, y2, y3 = (n1 // 8, 8, nt - 1, 8, LANES), (n2 // 8, 8, nt, 8, LANES), (ncols // 8, 8, nt, 8, LANES)
    y, stat, r, raw, wl = call(
        functools.partial(ahead_first, edge), 60000000, (f, low_in, high_in),
        (hds(*y1), sds(4, nt, n1, LANES), sds(nt - 1, n1, LANES), sds(18, n1, LANES), sds(24, LANES)),
        [vmem(9, nt, rows, LANES), vmem(9, nt, n1, LANES), strip, strip, vmem(*y1), dma(2), dma(n1 // 8)],
        weights=True, in_any=(1, 2), out_far=(0,),
    )
    dyn, r8, chunk, sums, mean = call(
        functools.partial(after_first, edge, ncols), 4000000, (wl, y, stat, raw, got, partner),
        (sds(5, nt, n1, LANES), sds(n1, LANES), sds(4, LANES), sds(4, LANES), sds(8, LANES)),
        [vmem(15, rows, LANES), vmem(*y1), dma(n1 // 8)], in_far=(1,),
    )

    def spread(chunk, sums):
        chunk = chunk + lax.ppermute(sums, "lat", swap)
        send = jnp.broadcast_to(chunk[None], (nlon, 4, LANES))
        return lax.all_to_all(send, "lon", 0, 0, tiled=True).reshape(nlon * 4, LANES)

    got = spread(chunk, sums)
    (y,) = call(
        functools.partial(ahead_later, 4), 50000000, (dyn, r, r8), (hds(*y2),),
        [vmem(8, nt, n1, LANES), vmem(8, nt, n2, LANES), vmem(*y2), dma(n2 // 8)], weights=True, out_far=(0,),
    )
    dyn, chunk, sums, mean = call(
        functools.partial(after_second, edge, ncols), 4000000, (wl, y, stat, r8, got, partner, mean),
        (sds(5, nt, n2, LANES), sds(4, LANES), sds(4, LANES), sds(8, LANES)), [vmem(12, rows, LANES), vmem(*y2), dma(n2 // 8)], in_far=(1,),
    )
    got = spread(chunk, sums)
    (y,) = call(
        functools.partial(ahead_later, 8), 40000000, (dyn, r, r8), (hds(*y3),),
        [vmem(8, nt, n2, LANES), vmem(8, nt, ncols, LANES), vmem(*y3), dma(ncols // 8)], weights=True, out_far=(0,),
    )
    return call(
        functools.partial(after_third, nrows), 4000000, (wl, y, r8, got, partner, mean),
        (hds(3, ncols, nrows), hds(ncols, nrows), sds(ITERS)),
        [vmem(12, rows, LANES), vmem(*y3), vmem(4, ncols, nrows), dma(ncols // 8), dma(ncols // 2)], in_far=(1,), out_far=(0, 1), scalars=(2,),
    )


def solution(mesh):
    in_specs = (
        P(None, "lon", "lat"),
        P(None, "lon", "lat"),
        P("lon", "lat"),
        P(("member", "lon"), "lat"),
        P("lon", "lat"),
        P(),
        P(),
    )
    out_specs = (P(None, ("member", "lon"), "lat"), P(("member", "lon"), "lat"), P("member"))
    return jax.shard_map(step, mesh=mesh, in_specs=in_specs, out_specs=out_specs, check_vma=False)
```
